256 devices in a mesh: groups: 2 (over z), patch: 128 (over x, y, core).
Axes of the slice: x: 8, y: 8, z: 2, core: 2. Of those that a mesh axis runs over, the one named last changes fastest.
The devices are a block of a 8x8x16 slice.
Arguments:
- grid_latents: bfloat16 [262144, 512], P(('groups', 'patch')), parts along dimension 0, may hold values from -6 to 6
- mesh_latents: bfloat16 [131072, 512], P(('groups', 'patch')), parts along dimension 0, may hold values from -6 to 6
- enc_send: int32 [5120, 128], P(('groups', 'patch')), parts along dimension 0, may hold values from 0 to 1023
- enc_recv: int32 [5120, 128], P(('groups', 'patch')), parts along dimension 0, may hold values from 0 to 512, as said below
- neighbours: int32 [131072, 32], P(('groups', 'patch')), parts along dimension 0, may hold values from 0 to 65535, as said below
- enc_grid_w: bfloat16 [512, 512], replicated, may hold values from -0.25 to 0.25
- enc_bias: float32 [512], replicated, may hold values from -4 to 4
- enc_mesh_w: bfloat16 [512, 512], replicated, may hold values from -0.25 to 0.25
- enc_msg_w: bfloat16 [512, 512], replicated, may hold values from -0.25 to 0.25
- upd_agg_w: bfloat16 [512, 512], replicated, may hold values from -0.25 to 0.25
- upd_mesh_w: bfloat16 [512, 512], replicated, may hold values from -0.25 to 0.25
- upd_out_w: bfloat16 [512, 512], replicated, may hold values from -0.25 to 0.25
- norm_gain: float32 [512], replicated, may hold values from 0.1 to 1.9
- query_w: bfloat16 [512, 512], replicated, may hold values from -0.25 to 0.25
- key_w: bfloat16 [512, 512], replicated, may hold values from -0.25 to 0.25
- value_w: bfloat16 [512, 512], replicated, may hold values from -0.25 to 0.25
- out_w: bfloat16 [512, 512], replicated, may hold values from -0.25 to 0.25
- ffn_gain: float32 [512], replicated, may hold values from 0.1 to 1.9
- ffn_in_w: bfloat16 [512, 2048], replicated, may hold values from -0.25 to 0.25
- ffn_out_w: bfloat16 [2048, 512], replicated, may hold values from -0.125 to 0.125
Outputs:
- result: bfloat16 [131072, 512], P(('groups', 'patch')), parts along dimension 0
The draws below stay inside these ranges and needn't reach their ends.
There are 2 independent parts, one for each index of `groups`. The reference program is written for one: setup_inputs(seed, part) draws one part's arguments, and reference() takes and returns one part's arrays. A program takes and returns all parts, laid end to end along the dimension named above; an argument that names none is the same for every part. Nothing has to cross between parts.
Inputs may be any that keep to these rules, and one draw needn't show every extreme that they name: `enc_recv`: in each band's slots for one owner, the used edges come first and the rest hold 512; the first and last bands fill all their slots. `neighbours`: neighbour 0 of a node is the node itself; every neighbour's owner is within 2 patch indices of the node's owner, wrapping around.
All inputs are finite; a program needn't handle non-finite values.
Results may differ from the reference program's by a relative error of at most 0.006.
The reference program's roundings to bfloat16 on the way count: a program that leaves them out, or rounds other values in their place, can miss the bound.
Values may be sent and summed in bfloat16 or wider, within the bound.
A program may use at most 256 MiB of HBM per device.

```python
import math
import jax
import jax.numpy as jnp
from jax import lax

D = 512
HEADS = 4
FF = 2048
G_DEV = 1024
M_DEV = 512
EB = 4
EDGE_BLOCK = 128
REACH = 2
KNB = 32
GRID = 131072
MESH = 65536
BLOCKS = 2560
N_PATCH = 128


def draw_enc_recv(key, part):
    capacity = EB * EDGE_BLOCK
    hop_count = 2 * REACH + 1
    devices = jnp.arange(N_PATCH, dtype=jnp.int32)
    distance = jnp.abs(2 * devices + 1 - N_PATCH)
    base_count = capacity // 2 + capacity // 2 * distance * distance // ((N_PATCH - 1) * (N_PATCH - 1))
    first_key, second_key = jax.random.split(key)
    removed = jax.random.randint(first_key, (N_PATCH, hop_count), 0, capacity // 16 + 1)
    removed = jnp.where((distance < N_PATCH - 1)[:, None], removed, 0)
    counts = base_count[:, None] - removed
    rows_drawn = jax.random.randint(second_key, (N_PATCH, hop_count, capacity), 0, M_DEV)
    slot_ids = jnp.arange(capacity, dtype=jnp.int32)
    filled = jnp.where(slot_ids[None, None, :] < counts[:, :, None], rows_drawn, M_DEV)
    return filled.astype(jnp.int32).reshape(N_PATCH * hop_count * EB, EDGE_BLOCK)


def draw_neighbours(key, part):
    node_ids = jnp.arange(MESH, dtype=jnp.int32)
    owners = node_ids // M_DEV
    first_key, second_key = jax.random.split(key)
    steps_drawn = jax.random.randint(first_key, (MESH, KNB), -REACH, REACH + 1)
    rows_drawn = jax.random.randint(second_key, (MESH, KNB), 0, M_DEV)
    others = (owners[:, None] + steps_drawn) % N_PATCH * M_DEV + rows_drawn
    leading = jnp.arange(KNB, dtype=jnp.int32)[None, :] == 0
    return jnp.where(leading, node_ids[:, None], others).astype(jnp.int32)


def place_ends(drawn, rng, smallest, high):
    spot = [jax.random.randint(jax.random.fold_in(rng, axis), (), 0, length) for axis, length in enumerate(drawn.shape)]
    main_axis = drawn.shape.index(max(drawn.shape))
    next_to = spot[:main_axis] + [(spot[main_axis] + 1) % drawn.shape[main_axis]] + spot[main_axis + 1:]
    return drawn.at[tuple(spot)].set(smallest).at[tuple(next_to)].set(high)


def block_scale(own_key, dims, cuts, smallest, high):
    level = 1.0
    for axis_at, parts in cuts:
        draws = jax.random.uniform(jax.random.fold_in(jax.random.fold_in(own_key, 6), axis_at), (parts,), jnp.float32, smallest / len(cuts), high / len(cuts))
        level = level * jnp.repeat(jnp.exp(draws), dims[axis_at] // parts).reshape((-1,) + (1,) * (len(dims) - 1 - axis_at))
    return level


def bell_draw(stream_key, dims, scale, most, shards=(), held_as=jnp.bfloat16):
    values = scale * jax.random.normal(stream_key, dims, jnp.float32)
    if shards:
        values = values * block_scale(stream_key, dims, shards, -0.22, 0.18)
    return jnp.clip(values, -most, most).astype(held_as)


def setup_inputs(seed: int = 0, part: int = 0) -> dict:
    streams_of = jax.random.split(jax.random.key(seed), 21)
    part_keys = jax.random.split(jax.random.fold_in(streams_of[20], part), 21)
    grid_latents = bell_draw(part_keys[0], (GRID, D), 1.0, 6.0, ((0, 128),))
    mesh_latents = bell_draw(part_keys[1], (MESH, D), 1.0, 6.0, ((0, 128),))
    enc_send = place_ends(jax.random.randint(part_keys[2], (BLOCKS, EDGE_BLOCK), 0, G_DEV), jax.random.fold_in(part_keys[2], 1), 0, G_DEV - 1).astype(jnp.int32)
    enc_recv = draw_enc_recv(jax.random.fold_in(jax.random.fold_in(streams_of[20], part), 71), part)
    neighbours = draw_neighbours(jax.random.fold_in(jax.random.fold_in(streams_of[20], part), 71), part)
    enc_grid_w = bell_draw(streams_of[5], (D, D), D ** -0.5, 0.25)
    enc_bias = bell_draw(streams_of[6], (D,), 1.0, 4.0, (), jnp.float32)
    enc_mesh_w = bell_draw(streams_of[7], (D, D), D ** -0.5, 0.25)
    enc_msg_w = bell_draw(streams_of[8], (D, D), D ** -0.5, 0.25)
    upd_agg_w = bell_draw(streams_of[9], (D, D), D ** -0.5, 0.25)
    upd_mesh_w = bell_draw(streams_of[10], (D, D), D ** -0.5, 0.25)
    upd_out_w = bell_draw(streams_of[11], (D, D), D ** -0.5, 0.25)
    norm_gain = jnp.clip(1.0 + 0.18 * jax.random.normal(streams_of[12], (D,), jnp.float32), 0.1, 1.9)
    query_w = bell_draw(streams_of[13], (D, D), D ** -0.5, 0.25)
    key_w = bell_draw(streams_of[14], (D, D), D ** -0.5, 0.25)
    value_w = bell_draw(streams_of[15], (D, D), D ** -0.5, 0.25)
    out_w = bell_draw(streams_of[16], (D, D), D ** -0.5, 0.25)
    ffn_gain = jnp.clip(1.0 + 0.18 * jax.random.normal(streams_of[17], (D,), jnp.float32), 0.1, 1.9)
    ffn_in_w = bell_draw(streams_of[18], (D, FF), D ** -0.5, 0.25)
    ffn_out_w = bell_draw(streams_of[19], (FF, D), FF ** -0.5, 0.125)
    return {"grid_latents": grid_latents, "mesh_latents": mesh_latents, "enc_send": enc_send, "enc_recv": enc_recv, "neighbours": neighbours, "enc_grid_w": enc_grid_w, "enc_bias": enc_bias, "enc_mesh_w": enc_mesh_w, "enc_msg_w": enc_msg_w, "upd_agg_w": upd_agg_w, "upd_mesh_w": upd_mesh_w, "upd_out_w": upd_out_w, "norm_gain": norm_gain, "query_w": query_w, "key_w": key_w, "value_w": value_w, "out_w": out_w, "ffn_gain": ffn_gain, "ffn_in_w": ffn_in_w, "ffn_out_w": ffn_out_w}


norm_eps = 1e-05
head_eps = 1e-06

def rms_scale(values, gain_vector):
    square = lax.optimization_barrier(jnp.mean(values * values, axis=-1, keepdims=True))
    return (values * lax.rsqrt(square + norm_eps) * gain_vector).astype(jnp.bfloat16)

def reference(grid_latents, mesh_latents, enc_send, enc_recv, neighbours, enc_grid_w, enc_bias, enc_mesh_w, enc_msg_w, upd_agg_w, upd_mesh_w, upd_out_w, norm_gain, query_w, key_w, value_w, out_w, ffn_gain, ffn_in_w, ffn_out_w):
    hop_count = 2 * REACH + 1
    capacity = EB * EDGE_BLOCK
    projected = (jnp.dot(grid_latents, enc_grid_w, preferred_element_type=jnp.float32) + enc_bias).astype(jnp.bfloat16)
    receiver_proj = jnp.dot(mesh_latents, enc_mesh_w, preferred_element_type=jnp.float32).astype(jnp.bfloat16)
    senders = enc_send.reshape(N_PATCH, hop_count, capacity)
    targets = enc_recv.reshape(N_PATCH, hop_count, capacity)
    devices = jnp.arange(N_PATCH, dtype=jnp.int32)[:, None, None]
    offsets = (jnp.arange(hop_count, dtype=jnp.int32) - REACH)[None, :, None]
    owners = (devices + offsets) % N_PATCH
    sender_ids = (devices * G_DEV + senders).reshape(N_PATCH, -1)
    receiver_ids = (owners * M_DEV + jnp.minimum(targets, M_DEV - 1)).reshape(N_PATCH, -1)
    segment_ids = jnp.where(targets < M_DEV, owners * M_DEV + targets, MESH).astype(jnp.int32).reshape(N_PATCH, -1)

    def add_device(summed, inputs):
        send_rows = jnp.take(projected, inputs[0], axis=0).astype(jnp.float32)
        recv_rows = jnp.take(receiver_proj, inputs[1], axis=0).astype(jnp.float32)
        active = jax.nn.silu(send_rows + recv_rows).astype(jnp.bfloat16)
        message = jnp.dot(active, enc_msg_w, preferred_element_type=jnp.float32).astype(jnp.bfloat16)
        return (summed + jax.ops.segment_sum(message.astype(jnp.float32), inputs[2], num_segments=MESH + 1), None)
    summed, _ = lax.scan(add_device, jnp.zeros((MESH + 1, D), jnp.float32), (sender_ids, receiver_ids, segment_ids))
    aggregate = summed[:MESH].astype(jnp.bfloat16)
    update = jax.nn.silu(jnp.dot(aggregate, upd_agg_w, preferred_element_type=jnp.float32) + jnp.dot(mesh_latents, upd_mesh_w, preferred_element_type=jnp.float32)).astype(jnp.bfloat16)
    encoded = mesh_latents.astype(jnp.float32) + jnp.dot(update, upd_out_w, preferred_element_type=jnp.float32)
    normed = rms_scale(encoded, norm_gain)
    queries = jnp.dot(normed, query_w, preferred_element_type=jnp.float32).astype(jnp.bfloat16)
    key_proj = jnp.dot(normed, key_w, preferred_element_type=jnp.float32).astype(jnp.bfloat16)
    values = jnp.dot(normed, value_w, preferred_element_type=jnp.float32).astype(jnp.bfloat16)
    head_size = D // HEADS

    def attend(inputs):
        block_queries, block_links = inputs
        row_count = block_queries.shape[0]
        neighbour_key_rows = jnp.take(key_proj, block_links.reshape(-1), axis=0).astype(jnp.float32).reshape(row_count, KNB, HEADS, head_size)
        neighbour_value_rows = jnp.take(values, block_links.reshape(-1), axis=0).astype(jnp.float32).reshape(row_count, KNB, HEADS, head_size)
        query_per_head = block_queries.astype(jnp.float32).reshape(row_count, HEADS, head_size)
        score_products = jnp.einsum('jou,jsou->jso', query_per_head, neighbour_key_rows)
        query_squares = jnp.einsum('tfe,tfe->tf', query_per_head, query_per_head)
        key_sq = jnp.einsum('mkhd,mkhd->mkh', neighbour_key_rows, neighbour_key_rows)
        scores = score_products * lax.rsqrt(query_squares / head_size + head_eps)[:, None, :] * lax.rsqrt(key_sq / head_size + head_eps) / math.sqrt(head_size)
        exponent = jnp.exp(scores)
        attention_weights = (exponent / lax.optimization_barrier(jnp.sum(exponent, axis=1, keepdims=True))).astype(jnp.bfloat16)
        attention_mixture = jnp.einsum('oia,oiae->oae', attention_weights.astype(jnp.float32), neighbour_value_rows)
        return attention_mixture.astype(jnp.bfloat16).reshape(row_count, D)
    attended = lax.map(attend, (queries.reshape(N_PATCH, M_DEV, D), neighbours.reshape(N_PATCH, M_DEV, KNB))).reshape(MESH, D)
    hidden = encoded + jnp.dot(attended, out_w, preferred_element_type=jnp.float32)
    normed_ffn = rms_scale(hidden, ffn_gain)
    expanded = jax.nn.silu(jnp.dot(normed_ffn, ffn_in_w, preferred_element_type=jnp.float32)).astype(jnp.bfloat16)
    return (hidden + jnp.dot(expanded, ffn_out_w, preferred_element_type=jnp.float32)).astype(jnp.bfloat16)
```

```python
import functools
import math

import jax
import jax.numpy as jnp
from jax import lax
from jax.experimental import pallas as pl
from jax.experimental.pallas import tpu as pltpu
from jax.sharding import PartitionSpec as P

HEADS = 4
REACH = 2
LANES = 128
CHUNK = 256

NORM_EPS = 1e-05
HEAD_EPS = 1e-06

OWN, SIB, OTH, FW, NF = range(5)
DELTA = {OWN: 0, SIB: 1, OTH: -1, FW: 2, NF: -2}
MIRROR = {SIB: SIB, OTH: OTH, FW: NF, NF: FW}

EDGE_SEND = [(FW, 0), (NF, 0), (FW, 1), (NF, 1), (OTH, 0), (OTH, 1), (SIB, 0), (SIB, 1), (OWN, 0), (OWN, 1)]
EDGE_USE = [(OWN, 0), (OWN, 1), (SIB, 0), (SIB, 1), (NF, 0), (FW, 0), (NF, 1), (FW, 1), (OTH, 0), (OTH, 1)]
EDGE_SLOT = {key: slot for slot, key in enumerate(EDGE_USE)}
NODE_USE = [(OWN, 0), (OWN, 1), (SIB, 0), (SIB, 1), (NF, 0), (FW, 0), (OTH, 0), (NF, 1), (FW, 1), (OTH, 1)]
NODE_SLOT = {key: slot for slot, key in enumerate(NODE_USE)}

f32 = jnp.float32
bf16 = jnp.bfloat16
i32 = jnp.int32


def dot(a, b):
    return jnp.dot(a, b, preferred_element_type=f32)


def dot_last(a, b):
    return lax.dot_general(a, b, (((1,), (1,)), ((), ())), preferred_element_type=f32)


def silu(x):
    half = 0.5 * x
    return half * jnp.tanh(half) + half


def flag(mask):
    return jnp.where(mask, 1.0, 0.0).astype(bf16)


def kernel(
    count,
    grid_hbm, mesh_hbm, send_ref, recv_ref, neigh_ref,
    grid_w_hbm, bias_ref, mesh_w_hbm, msg_w_hbm, upd_agg_hbm, upd_mesh_hbm, upd_out_hbm,
    gain_ref, query_hbm, key_hbm, value_hbm, out_w_hbm, ffn_gain_ref, ffn_in_hbm, ffn_out_hbm,
    result_ref,
    grid_v, mesh_v, grid_w, mesh_w, msg_w, upd_agg, upd_mesh, upd_out, query_w, key_w, value_w, out_w, ffn_in, ffn_out,
    projected, receiver, base, summed, encoded, edges, nodes, counts, queries, values, mixed,
    send_cols, land_cols, land_rows, stage, land_send, land_recv, hi_tiled, lo_tiled,
    load_sem, ls_sem, lr_sem, es_sem, er_sem, ns_sem, nr_sem,
):
    me = lax.axis_index("patch")
    sign = 1 - 2 * (me % 2)
    device = {role: (me + sign * DELTA[role] + count) % count for role in DELTA}
    block_row = {role: 4 * (sign * DELTA[role] + REACH) for role in DELTA}
    rows = mesh_v.shape[0]

    def load(index, src, dst):
        copy = pltpu.make_async_copy(src, dst, load_sem.at[index])
        copy.start()
        return copy

    def remote(src, dst, send_sem, recv_sem, role):
        return pltpu.make_async_remote_copy(
            src_ref=src, dst_ref=dst, send_sem=send_sem, recv_sem=recv_sem,
            device_id={"patch": device[role]}, device_id_type=pl.DeviceIdType.MESH,
        )

    pairs = [
        (grid_hbm, grid_v), (grid_w_hbm, grid_w), (mesh_hbm, mesh_v), (mesh_w_hbm, mesh_w), (msg_w_hbm, msg_w),
        (upd_mesh_hbm, upd_mesh), (upd_agg_hbm, upd_agg), (upd_out_hbm, upd_out), (query_hbm, query_w),
        (key_hbm, key_w), (value_hbm, value_w), (out_w_hbm, out_w), (ffn_in_hbm, ffn_in), (ffn_out_hbm, ffn_out),
    ]
    loads = [load(index, src, dst) for index, (src, dst) in enumerate(pairs)]

    barrier = pltpu.get_barrier_semaphore()
    for role in (SIB, OTH, FW, NF):
        pl.semaphore_signal(
            barrier, inc=1, device_id={"patch": device[role]}, device_id_type=pl.DeviceIdType.MESH
        )

    land_send[...] = jnp.zeros_like(land_send)
    stage[...] = jnp.zeros_like(stage)
    for role in DELTA:
        for j in range(4):
            land_send[role, j : j + 1, :] = recv_ref[pl.ds(block_row[role] + j, 1), :]
    for k, (role, half) in enumerate(EDGE_SEND):
        for j in range(2):
            stage[2 * k + j : 2 * k + j + 1, :] = send_ref[pl.ds(block_row[role] + 2 * half + j, 1), :]

    pl.semaphore_wait(barrier, 4)
    land_copies = []
    for role in (SIB, OTH, FW, NF):
        copy = remote(
            land_send.at[role], land_recv.at[MIRROR[role]], ls_sem.at[role - 1], lr_sem.at[MIRROR[role] - 1], role
        )
        copy.start()
        land_copies.append(copy)

    turned = stage[...].T
    for b in range(20):
        send_cols[b] = jnp.broadcast_to(turned[:, b : b + 1], (LANES, LANES))

    lane = lax.broadcasted_iota(i32, (CHUNK, LANES), 1)

    def onehot(cols, k, width):
        col = jnp.concatenate([cols[2 * k], cols[2 * k + 1]], axis=0)
        return jnp.concatenate([flag(col == lane + LANES * t) for t in range(width // LANES)], axis=1)

    loads[0].wait()
    loads[1].wait()

    def project(t, carry):
        at = pl.ds(pl.multiple_of(t * CHUNK, CHUNK), CHUNK)
        projected[at, :] = (dot(grid_v[at, :], grid_w[...]) + bias_ref[...]).astype(bf16)
        return carry

    lax.fori_loop(0, grid_v.shape[0] // CHUNK, project, 0)

    def edge_copy(k):
        role, half = EDGE_SEND[k]
        slot = EDGE_SLOT[(MIRROR[role], half)]
        return remote(edges.at[10 + k], edges.at[slot], es_sem.at[k], er_sem.at[slot - 2], role)

    def pick(k, carry):
        chosen = onehot(send_cols, k, grid_v.shape[0])
        edges[(10 + k) % 18] = dot(chosen, projected[...]).astype(bf16)
        for index in range(8):
            @pl.when(k == index)
            def _():
                edge_copy(index).start()
        return carry

    lax.fori_loop(0, 10, pick, 0)

    loads[2].wait()
    loads[3].wait()
    loads[5].wait()

    def prepare(t, carry):
        at = pl.ds(pl.multiple_of(t * CHUNK, CHUNK), CHUNK)
        latents = mesh_v[at, :]
        receiver[at, :] = dot(latents, mesh_w[...]).astype(bf16)
        base[at, :] = dot(latents, upd_mesh[...])
        summed[at, :] = jnp.zeros((CHUNK, summed.shape[1]), f32)
        return carry

    lax.fori_loop(0, rows // CHUNK, prepare, 0)

    for role in (SIB, OTH, FW, NF):
        remote(land_send.at[role], land_recv.at[role], ls_sem.at[role - 1], lr_sem.at[role - 1], role).wait_recv()
    for i, (role, half) in enumerate(EDGE_USE):
        source = land_send if role == OWN else land_recv
        for j in range(2):
            row = source[role, 2 * half + j : 2 * half + j + 1, :]
            land_rows[2 * i + j] = row
            stage[2 * i + j : 2 * i + j + 1, :] = row
    landed = stage[...].T
    for b in range(20):
        land_cols[b] = jnp.broadcast_to(landed[:, b : b + 1], (LANES, LANES))
    loads[4].wait()

    def use_edges(i):
        receiver_rows = dot(onehot(land_cols, i, rows), receiver[...])
        active = silu(edges[i].astype(f32) + receiver_rows).astype(bf16)
        message = dot(active, msg_w[...]).astype(bf16)
        landing = jnp.concatenate([land_rows[2 * i], land_rows[2 * i + 1]], axis=1)
        scatter = flag(lax.broadcasted_iota(i32, (rows, CHUNK), 0) == landing)
        summed[...] += dot(scatter, message)

    def own_edges(i, carry):
        use_edges(i)
        return carry

    lax.fori_loop(0, 2, own_edges, 0)

    neigh = neigh_ref[...]
    owner = lax.div(neigh, i32(rows))
    row = lax.rem(neigh, i32(rows))
    step = lax.rem((owner - me) * sign + 2 * count, i32(count))
    half = lax.div(row, i32(CHUNK))
    near = jnp.where(step == 0, half, 2 + half)
    far = jnp.where(step == count - 2, 4, jnp.where(step == 2, 5, 6)) + 3 * half
    slot = jnp.where(step <= 1, near, far)
    high = 2 * slot + lax.rem(lax.div(row, i32(LANES)), i32(2))
    low = lax.rem(row, i32(LANES))
    links = neigh.shape[1]
    spread = flag(
        lax.rem(lax.broadcasted_iota(i32, (links, LANES), 1), i32(links))
        == lax.broadcasted_iota(i32, (links, LANES), 0)
    )
    hi_tiled[...] = dot(high.astype(f32).astype(bf16), spread)
    lo_tiled[...] = dot(low.astype(f32).astype(bf16), spread)
    sub8 = lax.broadcasted_iota(i32, (8, LANES), 0)
    piece = lax.div(lax.broadcasted_iota(i32, (8, LANES), 1), i32(links))
    first = piece == sub8
    second = piece + LANES // links == sub8
    low_id = lax.broadcasted_iota(i32, (LANES, 2 * LANES), 0).astype(f32)

    def count_group(g, carry):
        at = pl.ds(pl.multiple_of(8 * g, 8), 8)
        h8, l8 = hi_tiled[at, :], lo_tiled[at, :]
        key = jnp.concatenate([jnp.where(first, h8, -1.0), jnp.where(second, h8, -1.0)], axis=1)
        by_high = jnp.concatenate([jnp.where(key == float(v), 1.0, 0.0) for v in range(20)], axis=0).astype(bf16)
        low_row = jnp.concatenate(
            [
                jnp.sum(jnp.where(first, l8, 0.0), axis=0, keepdims=True),
                jnp.sum(jnp.where(second, l8, 0.0), axis=0, keepdims=True),
            ],
            axis=1,
        )
        by_low = flag(low_id == low_row)
        found = dot_last(by_high, by_low)
        for v in range(20):
            counts[v // 2, at, (v % 2) * LANES : (v % 2 + 1) * LANES] = found[8 * v : 8 * v + 8, :]
        return carry

    lax.fori_loop(0, rows // 8, count_group, 0, unroll=2)

    def far_edges(i, carry):
        pltpu.make_async_remote_copy(
            src_ref=edges.at[i], dst_ref=edges.at[i], send_sem=es_sem.at[0], recv_sem=er_sem.at[i - 2],
            device_id={"patch": device[SIB]}, device_id_type=pl.DeviceIdType.MESH,
        ).wait_recv()
        use_edges(i)
        return carry

    lax.fori_loop(2, 10, far_edges, 0)

    for index in (6, 7, 8):
        loads[index].wait()

    def node_copy(index, role, half):
        slot = NODE_SLOT[(MIRROR[role], half)]
        return remote(
            nodes.at[NODE_SLOT[(OWN, half)]], nodes.at[slot], ns_sem.at[index], nr_sem.at[slot - 2], role
        )

    head = rows // HEADS
    query_scale = math.log2(math.e) / math.sqrt(head)

    def unit(x, scale):
        parts = []
        for h in range(HEADS):
            part = x[:, h * head : (h + 1) * head]
            square = jnp.mean(part * part, axis=-1, keepdims=True)
            parts.append((part * (lax.rsqrt(square + HEAD_EPS) * scale)).astype(bf16))
        return jnp.concatenate(parts, axis=1)

    def rms_scale(x, gain):
        square = jnp.mean(x * x, axis=-1, keepdims=True)
        return (x * lax.rsqrt(square + NORM_EPS) * gain).astype(bf16)

    node_copies = []
    for c in range(2):
        at = slice(c * CHUNK, (c + 1) * CHUNK)
        update = silu(dot(summed[at, :].astype(bf16), upd_agg[...]) + base[at, :]).astype(bf16)
        latent = mesh_v[at, :].astype(f32) + dot(update, upd_out[...])
        encoded[at, :] = latent
        nodes[c] = rms_scale(latent, gain_ref[...])
        for index, role in enumerate((NF, FW, SIB)):
            copy = node_copy(3 * c + index, role, c)
            copy.start()
            node_copies.append(copy)
    for c in range(2):
        at = slice(c * CHUNK, (c + 1) * CHUNK)
        queries[at, :] = unit(dot(nodes[c], query_w[...]), query_scale)
    mixed[...] = jnp.zeros_like(mixed)
    values[...] = jnp.ones_like(values)
    loads[9].wait()
    loads[10].wait()

    def pass_on(half):
        source = NODE_SLOT[(FW, half)]
        slot = NODE_SLOT[(OTH, half)]
        return remote(nodes.at[source], nodes.at[slot], ns_sem.at[6 + half], nr_sem.at[slot - 2], SIB)

    def arrived(slot):
        remote(nodes.at[slot], nodes.at[slot], ns_sem.at[0], nr_sem.at[slot - 2], SIB).wait_recv()

    def attend(i, carry):
        for role, half in NODE_USE[2:]:
            index = NODE_SLOT[(role, half)]
            if role == FW:
                continue

            @pl.when(i == index)
            def _():
                if role == NF:
                    arrived(NODE_SLOT[(FW, half)])
                    pass_on(half).start()
                arrived(index)

        features = nodes[i]
        keys = unit(dot(features, key_w[...]), 1.0)
        value = dot(features, value_w[...]).astype(bf16)
        for h in range(HEADS):
            values[:, 2 * h * head : (2 * h + 1) * head] = value[:, h * head : (h + 1) * head]
        for t in range(rows // CHUNK):
            at = slice(t * CHUNK, (t + 1) * CHUNK)
            often = counts[i, at, :]
            for h in range(HEADS):
                cols = slice(h * head, (h + 1) * head)
                score = dot_last(queries[at, cols], keys[:, cols])
                weight = (jnp.exp2(score) * often).astype(bf16)
                wide = slice(2 * h * head, 2 * (h + 1) * head)
                mixed[at, wide] += dot(weight, values[:, wide])
        return carry

    lax.fori_loop(0, 10, attend, 0)

    for index in (11, 12, 13):
        loads[index].wait()

    def finish(t, carry):
        at = pl.ds(pl.multiple_of(t * CHUNK, CHUNK), CHUNK)
        attended = jnp.concatenate(
            [
                mixed[at, 2 * h * head : (2 * h + 1) * head] / mixed[at, (2 * h + 1) * head : 2 * (h + 1) * head]
                for h in range(HEADS)
            ],
            axis=1,
        ).astype(bf16)
        hidden = encoded[at, :] + dot(attended, out_w[...])
        normed = rms_scale(hidden, ffn_gain_ref[...])
        for c in range(ffn_in.shape[1] // 512):
            cols = slice(512 * c, 512 * (c + 1))
            expanded = silu(dot(normed, ffn_in[:, cols])).astype(bf16)
            hidden = hidden + dot(expanded, ffn_out[cols, :])
        result_ref[at, :] = hidden.astype(bf16)
        return carry

    lax.fori_loop(0, rows // CHUNK, finish, 0)

    for copy in land_copies + [edge_copy(k) for k in range(8)] + node_copies + [pass_on(0), pass_on(1)]:
        copy.wait_send()


def shards(
    grid_latents, mesh_latents, enc_send, enc_recv, neighbours,
    enc_grid_w, enc_bias, enc_mesh_w, enc_msg_w, upd_agg_w, upd_mesh_w, upd_out_w,
    norm_gain, query_w, key_w, value_w, out_w, ffn_gain, ffn_in_w, ffn_out_w,
):
    count = lax.axis_size("patch")
    rows, width = mesh_latents.shape
    any_spec = pl.BlockSpec(memory_space=pl.ANY)
    vmem_spec = pl.BlockSpec(memory_space=pltpu.VMEM)
    square = pltpu.VMEM((width, width), bf16)
    args = (
        grid_latents, mesh_latents, enc_send, enc_recv, neighbours,
        enc_grid_w, enc_bias[None, :], enc_mesh_w, enc_msg_w, upd_agg_w, upd_mesh_w, upd_out_w,
        norm_gain[None, :], query_w, key_w, value_w, out_w, ffn_gain[None, :], ffn_in_w, ffn_out_w,
    )
    in_vmem = {2, 3, 4, 6, 12, 17}
    return pl.pallas_call(
        functools.partial(kernel, count),
        out_shape=jax.ShapeDtypeStruct((rows, width), bf16),
        in_specs=[vmem_spec if index in in_vmem else any_spec for index in range(len(args))],
        out_specs=vmem_spec,
        scratch_shapes=[
            pltpu.VMEM(grid_latents.shape, bf16),
            pltpu.VMEM((rows, width), bf16),
            *([square] * 10),
            pltpu.VMEM(ffn_in_w.shape, bf16),
            pltpu.VMEM(ffn_out_w.shape, bf16),
            pltpu.VMEM(grid_latents.shape, bf16),
            pltpu.VMEM((rows, width), bf16),
            pltpu.VMEM((rows, width), f32),
            pltpu.VMEM((rows, width), f32),
            pltpu.VMEM((rows, width), f32),
            pltpu.VMEM((18, CHUNK, width), bf16),
            pltpu.VMEM((10, CHUNK, width), bf16),
            pltpu.VMEM((10, rows, CHUNK), f32),
            pltpu.VMEM((rows, width), bf16),
            pltpu.VMEM((CHUNK, 2 * width), bf16),
            pltpu.VMEM((rows, 2 * width), f32),
            pltpu.VMEM((20, LANES, LANES), i32),
            pltpu.VMEM((20, LANES, LANES), i32),
            pltpu.VMEM((20, 1, LANES), i32),
            pltpu.VMEM((LANES, LANES), i32),
            pltpu.VMEM((5, 8, LANES), i32),
            pltpu.VMEM((5, 8, LANES), i32),
            pltpu.VMEM((rows, LANES), f32),
            pltpu.VMEM((rows, LANES), f32),
            pltpu.SemaphoreType.DMA((14,)),
            pltpu.SemaphoreType.DMA((4,)),
            pltpu.SemaphoreType.DMA((4,)),
            pltpu.SemaphoreType.DMA((8,)),
            pltpu.SemaphoreType.DMA((8,)),
            pltpu.SemaphoreType.DMA((8,)),
            pltpu.SemaphoreType.DMA((8,)),
        ],
        compiler_params=pltpu.CompilerParams(
            collective_id=0, has_side_effects=True, vmem_limit_bytes=60 * 2**20
        ),
        name="encode_attend",
    )(*args)


def solution(mesh):
    split = P(("groups", "patch"), None)
    in_specs = (split,) * 5 + (P(),) * 15
    return jax.shard_map(shards, mesh=mesh, in_specs=in_specs, out_specs=split, check_vma=False)
```

```python
import functools
import math

import jax
import jax.numpy as jnp
from jax import lax
from jax.experimental import pallas as pl
from jax.experimental.pallas import tpu as pltpu
from jax.sharding import PartitionSpec as P

HEADS = 4
REACH = 2
LANES = 128
CHUNK = 256

NORM_EPS = 1e-05
HEAD_EPS = 1e-06

OWN, SIB, OTH, FW, NF = range(5)
DELTA = {OWN: 0, SIB: 1, OTH: -1, FW: 2, NF: -2}
MIRROR = {SIB: SIB, OTH: OTH, FW: NF, NF: FW}

EDGE_SEND = [(FW, 0), (NF, 0), (FW, 1), (NF, 1), (OTH, 0), (OTH, 1), (SIB, 0), (SIB, 1), (OWN, 0), (OWN, 1)]
EDGE_USE = [(OWN, 0), (OWN, 1), (SIB, 0), (SIB, 1), (NF, 0), (FW, 0), (NF, 1), (FW, 1), (OTH, 0), (OTH, 1)]
EDGE_SLOT = {key: slot for slot, key in enumerate(EDGE_USE)}
NODE_USE = (
    [(OWN, q) for q in range(4)] + [(SIB, q) for q in range(4)]
    + [(FW, 0), (FW, 1), (OTH, 0), (OTH, 1), (FW, 2), (NF, 0)]
    + [(FW, 3), (OTH, 2), (OTH, 3), (NF, 1), (NF, 2), (NF, 3)]
)
NODE_SLOT = {key: slot for slot, key in enumerate(NODE_USE)}

f32 = jnp.float32
bf16 = jnp.bfloat16
i32 = jnp.int32


def dot(a, b):
    return jnp.dot(a, b, preferred_element_type=f32)


def dot_last(a, b):
    return lax.dot_general(a, b, (((1,), (1,)), ((), ())), preferred_element_type=f32)


def dot_first(a, b):
    return lax.dot_general(a, b, (((0,), (0,)), ((), ())), preferred_element_type=f32)


def silu(x):
    half = 0.5 * x
    return half * jnp.tanh(half) + half


def flag(mask):
    return jnp.where(mask, 1.0, 0.0).astype(bf16)


def kernel(
    count,
    grid_hbm, mesh_hbm, send_hbm, recv_hbm, neigh_hbm,
    grid_w_hbm, bias_hbm, mesh_w_hbm, msg_w_hbm, upd_agg_hbm, upd_mesh_hbm, upd_out_hbm,
    gain_hbm, query_hbm, key_hbm, value_hbm, out_w_hbm, ffn_gain_hbm, ffn_in_hbm, ffn_out_hbm,
    result_ref,
    grid_v, mesh_v, send_ref, recv_ref, neigh_ref, bias_ref, gain_ref, ffn_gain_ref, grid_w, mesh_w, msg_w, upd_agg, upd_mesh, upd_out, query_w, key_w, value_w, out_w, ffn_in, ffn_out,
    projected, receiver, received, base, summed, encoded, edges, nodes, counts, queries, values, mixed,
    send_cols, land_cols, land_rows, stage, land_send, land_recv, hi_tiled, lo_rows, expanded,
    load_sem, ls_sem, lr_sem, es_sem, er_sem, ns_sem, nr_sem,
):
    me = lax.axis_index("patch")
    sign = 1 - 2 * (me % 2)
    device = {role: (me + sign * DELTA[role] + count) % count for role in DELTA}
    block_row = {role: 4 * (sign * DELTA[role] + REACH) for role in DELTA}
    rows = mesh_v.shape[0]

    def load(index, src, dst):
        copy = pltpu.make_async_copy(src, dst, load_sem.at[index])
        copy.start()
        return copy

    def remote(src, dst, send_sem, recv_sem, role):
        return pltpu.make_async_remote_copy(
            src_ref=src, dst_ref=dst, send_sem=send_sem, recv_sem=recv_sem,
            device_id={"patch": device[role]}, device_id_type=pl.DeviceIdType.MESH,
        )

    pairs = [
        (send_hbm, send_ref), (recv_hbm, recv_ref), (bias_hbm, bias_ref), (grid_hbm, grid_v), (grid_w_hbm, grid_w), (mesh_hbm, mesh_v), (mesh_w_hbm, mesh_w), (msg_w_hbm, msg_w),
        (upd_mesh_hbm, upd_mesh), (upd_agg_hbm, upd_agg), (upd_out_hbm, upd_out), (query_hbm, query_w),
        (gain_hbm, gain_ref), (ffn_gain_hbm, ffn_gain_ref), (neigh_hbm, neigh_ref), (key_hbm, key_w), (value_hbm, value_w), (out_w_hbm, out_w), (ffn_in_hbm, ffn_in), (ffn_out_hbm, ffn_out),
    ]
    loads = {id(dst): load(index, src, dst) for index, (src, dst) in enumerate(pairs[:5])}

    def wait_for(*refs):
        for ref in refs:
            loads[id(ref)].wait()

    barrier = pltpu.get_barrier_semaphore()
    for role in (SIB, OTH, FW, NF):
        pl.semaphore_signal(
            barrier, inc=1, device_id={"patch": device[role]}, device_id_type=pl.DeviceIdType.MESH
        )

    wait_for(send_ref, recv_ref)

    land_send[...] = jnp.zeros_like(land_send)
    stage[...] = jnp.zeros_like(stage)
    for role in DELTA:
        for j in range(4):
            land_send[role, j : j + 1, :] = recv_ref[pl.ds(block_row[role] + j, 1), :]
    for k, (role, half) in enumerate(EDGE_SEND):
        for j in range(2):
            stage[2 * k + j : 2 * k + j + 1, :] = send_ref[pl.ds(block_row[role] + 2 * half + j, 1), :]

    land_copies = [
        remote(land_send.at[role], land_recv.at[MIRROR[role]], ls_sem.at[role - 1], lr_sem.at[MIRROR[role] - 1], role)
        for role in (SIB, OTH, FW, NF)
    ]

    turned = stage[...].T
    for b in range(20):
        send_cols[b] = jnp.broadcast_to(turned[:, b : b + 1], (LANES, LANES))

    lane = lax.broadcasted_iota(i32, (CHUNK, LANES), 1)

    def onehot(cols, k, width):
        col = jnp.concatenate([cols[2 * k], cols[2 * k + 1]], axis=0)
        return jnp.concatenate([flag(col == lane + LANES * t) for t in range(width // LANES)], axis=1)

    with jax.named_scope("wait_grid"):
        wait_for(grid_v, grid_w, bias_ref)
    loads |= {id(dst): load(index + 5, src, dst) for index, (src, dst) in enumerate(pairs[5:])}

    def project(t, carry):
        at = pl.ds(pl.multiple_of(t * rows, rows), rows)
        projected[at, :] = (dot(grid_v[at, :], grid_w[...]) + bias_ref[...]).astype(bf16)
        return carry

    with jax.named_scope("project"):
        lax.fori_loop(0, grid_v.shape[0] // rows, project, 0)

    def edge_copy(k):
        role, half = EDGE_SEND[k]
        slot = EDGE_SLOT[(MIRROR[role], half)]
        return remote(edges.at[10 + k], edges.at[slot], es_sem.at[k], er_sem.at[slot - 2], role)

    def pick(k, carry):
        chosen = onehot(send_cols, k, grid_v.shape[0])
        edges[(10 + k) % 18] = dot(chosen, projected[...]).astype(bf16)

        @pl.when(k == 0)
        def _():
            pl.semaphore_wait(barrier, 4)
            for copy in land_copies:
                copy.start()

        for index in range(8):
            @pl.when(k == index)
            def _():
                edge_copy(index).start()
        return carry

    with jax.named_scope("pick"):
        lax.fori_loop(0, 10, pick, 0)

    wait_for(mesh_v, mesh_w, upd_mesh)

    def prepare(t, carry):
        at = pl.ds(pl.multiple_of(t * CHUNK, CHUNK), CHUNK)
        latents = mesh_v[at, :]
        receiver[at, :] = dot(latents, mesh_w[...]).astype(bf16)
        base[at, :] = dot(latents, upd_mesh[...])
        summed[at, :] = jnp.zeros((CHUNK, summed.shape[1]), f32)
        return carry

    with jax.named_scope("prepare"):
        lax.fori_loop(0, rows // CHUNK, prepare, 0)

    for role in (SIB, OTH, FW, NF):
        remote(land_send.at[role], land_recv.at[role], ls_sem.at[role - 1], lr_sem.at[role - 1], role).wait_recv()
    for i, (role, half) in enumerate(EDGE_USE):
        source = land_send if role == OWN else land_recv
        for j in range(2):
            row = source[role, 2 * half + j : 2 * half + j + 1, :]
            land_rows[2 * i + j] = row
            stage[2 * i + j : 2 * i + j + 1, :] = row
    landed = stage[...].T
    for b in range(20):
        land_cols[b] = jnp.broadcast_to(landed[:, b : b + 1], (LANES, LANES))
    wait_for(msg_w)

    def receive(i, carry):
        received[i] = dot(onehot(land_cols, i, rows), receiver[...]).astype(bf16)
        return carry

    def use_edges(i):
        active = silu(edges[i].astype(f32) + received[i].astype(f32)).astype(bf16)
        message = dot(active, msg_w[...]).astype(bf16)
        landing = jnp.concatenate([land_rows[2 * i], land_rows[2 * i + 1]], axis=1)
        scatter = flag(lax.broadcasted_iota(i32, (rows, CHUNK), 0) == landing)
        summed[...] += dot(scatter, message)

    def own_edges(i, carry):
        use_edges(i)
        return carry

    with jax.named_scope("receive"):
        lax.fori_loop(0, 10, receive, 0)
    with jax.named_scope("own_edges"):
        lax.fori_loop(0, 2, own_edges, 0)

    wait_for(neigh_ref)
    neigh = neigh_ref[...]
    owner = lax.div(neigh, i32(rows))
    row = lax.rem(neigh, i32(rows))
    step = lax.rem((owner - me) * sign + 2 * count, i32(count))
    quarter = lax.div(row, i32(LANES))
    far = jnp.zeros_like(quarter)
    for role, offset in ((FW, 2), (NF, count - 2), (OTH, count - 1)):
        for q in range(4):
            far = jnp.where((step == offset) & (quarter == q), NODE_SLOT[(role, q)], far)
    high = jnp.where(step <= 1, quarter + 4 * step, far)
    low = lax.rem(row, i32(LANES))
    links = neigh.shape[0]
    spread = flag(
        lax.rem(lax.broadcasted_iota(i32, (links, LANES), 1), i32(links))
        == lax.broadcasted_iota(i32, (links, LANES), 0)
    )
    hi_tiled[...] = dot_first(high.astype(f32).astype(bf16), spread)
    lo_tiled = dot_first(low.astype(f32).astype(bf16), spread)
    place = lax.rem(lax.broadcasted_iota(i32, (rows, LANES), 0), i32(8))
    node_piece = lax.div(lax.broadcasted_iota(i32, (rows, LANES), 1), i32(links))
    alone = jnp.concatenate(
        [
            jnp.where(node_piece == place, lo_tiled, 0.0).astype(bf16),
            jnp.where(node_piece + LANES // links == place, lo_tiled, 0.0).astype(bf16),
        ],
        axis=1,
    )
    group = flag(
        lax.div(lax.broadcasted_iota(i32, (rows // 8, rows), 1), i32(8))
        == lax.broadcasted_iota(i32, (rows // 8, rows), 0)
    )
    lo_rows[...] = dot(group, alone)
    sub8 = lax.broadcasted_iota(i32, (8, LANES), 0)
    piece = lax.div(lax.broadcasted_iota(i32, (8, LANES), 1), i32(links))
    first = piece == sub8
    second = piece + LANES // links == sub8
    low_id = lax.broadcasted_iota(i32, (LANES, 2 * LANES), 0).astype(f32)

    def count_group(g, carry):
        at = pl.ds(pl.multiple_of(8 * g, 8), 8)
        h8 = hi_tiled[at, :]
        key = jnp.concatenate([jnp.where(first, h8, -1.0), jnp.where(second, h8, -1.0)], axis=1)
        by_high = jnp.concatenate([jnp.where(key == float(v), 1.0, 0.0) for v in range(20)], axis=0).astype(bf16)
        by_low = flag(low_id == lo_rows[pl.ds(g, 1), :])
        found = dot_last(by_high, by_low)
        for v in range(20):
            counts[v // 2, at, (v % 2) * LANES : (v % 2 + 1) * LANES] = found[8 * v : 8 * v + 8, :]
        return carry

    with jax.named_scope("count"):
        lax.fori_loop(0, rows // 8, count_group, 0, unroll=4)

    def far_edges(i, carry):
        arrival = pltpu.make_async_remote_copy(
            src_ref=edges.at[i], dst_ref=edges.at[i], send_sem=es_sem.at[0], recv_sem=er_sem.at[i - 2],
            device_id={"patch": device[SIB]}, device_id_type=pl.DeviceIdType.MESH,
        )
        with jax.named_scope("wait_edges"):
            arrival.wait_recv()
        with jax.named_scope("use_edges"):
            use_edges(i)
        return carry

    with jax.named_scope("far_edges"):
        lax.fori_loop(2, 10, far_edges, 0)

    wait_for(upd_agg, upd_out, query_w, gain_ref)

    def node_copy(index, role, q):
        slot = NODE_SLOT[(MIRROR[role], q)]
        return remote(nodes.at[NODE_SLOT[(OWN, q)]], nodes.at[slot], ns_sem.at[index], nr_sem.at[slot - 4], role)

    head = rows // HEADS
    query_scale = math.log2(math.e) / math.sqrt(head)

    def unit(x, scale):
        parts = []
        for h in range(HEADS):
            part = x[:, h * head : (h + 1) * head]
            square = jnp.mean(part * part, axis=-1, keepdims=True)
            parts.append((part * (lax.rsqrt(square + HEAD_EPS) * scale)).astype(bf16))
        return jnp.concatenate(parts, axis=1)

    def rms_scale(x, gain):
        square = jnp.mean(x * x, axis=-1, keepdims=True)
        return (x * lax.rsqrt(square + NORM_EPS) * gain).astype(bf16)

    node_copies = []
    for c in range(2):
        with jax.named_scope("update"):
            at = slice(c * CHUNK, (c + 1) * CHUNK)
            update = silu(dot(summed[at, :].astype(bf16), upd_agg[...]) + base[at, :]).astype(bf16)
            latent = mesh_v[at, :].astype(f32) + dot(update, upd_out[...])
            encoded[at, :] = latent
            normed = rms_scale(latent, gain_ref[...])
            for q in (2 * c, 2 * c + 1):
                nodes[q] = normed[(q - 2 * c) * LANES : (q - 2 * c + 1) * LANES, :]
                node_copies += [node_copy(3 * q + index, role, q) for index, role in enumerate((NF, SIB, FW))]
                for copy in node_copies[-3:-1]:
                    copy.start()
    with jax.named_scope("queries"):
        for c in range(2):
            at = slice(c * CHUNK, (c + 1) * CHUNK)
            own = jnp.concatenate([nodes[2 * c], nodes[2 * c + 1]], axis=0)
            queries[at, :] = unit(dot(own, query_w[...]), query_scale)
    mixed[...] = jnp.zeros_like(mixed)
    values[...] = jnp.ones_like(values)
    wait_for(key_w, value_w)

    def pass_on(q):
        source, slot = NODE_SLOT[(FW, q)], NODE_SLOT[(OTH, q)]
        return remote(nodes.at[source], nodes.at[slot], ns_sem.at[12 + q], nr_sem.at[slot - 4], SIB)

    def arrived(slot):
        remote(nodes.at[slot], nodes.at[slot], ns_sem.at[0], nr_sem.at[slot - 4], SIB).wait_recv()

    def wait_nodes(i):
        for step_index in range(2, 10):
            @pl.when(i == step_index)
            def _():
                pair = NODE_USE[2 * step_index : 2 * step_index + 2]
                for role, q in sorted(pair, key=lambda block: block[0] != FW):
                    arrived(NODE_SLOT[(role, q)])
                    if role == FW:
                        pass_on(q).start()

    def attend(i, carry):
        for step_index in (1, 2):
            @pl.when(i == step_index)
            def _():
                for q in (2 * step_index - 2, 2 * step_index - 1):
                    node_copies[3 * q + 2].start()

        with jax.named_scope("wait_nodes"):
            wait_nodes(i)
        with jax.named_scope("attend_one"):
            attend_one(i)
        return carry

    def attend_one(i):
        features = jnp.concatenate([nodes[2 * i], nodes[2 * i + 1]], axis=0)
        keys = unit(dot(features, key_w[...]), 1.0)
        value = dot(features, value_w[...]).astype(bf16)
        for h in range(HEADS):
            values[:, 2 * h * head : (2 * h + 1) * head] = value[:, h * head : (h + 1) * head]
        for t in range(rows // CHUNK):
            at = slice(t * CHUNK, (t + 1) * CHUNK)
            often = counts[i, at, :]
            for h in range(HEADS):
                cols = slice(h * head, (h + 1) * head)
                score = dot_last(queries[at, cols], keys[:, cols])
                weight = (jnp.exp2(score) * often).astype(bf16)
                wide = slice(2 * h * head, 2 * (h + 1) * head)
                mixed[at, wide] += dot(weight, values[:, wide])

    with jax.named_scope("attend"):
        lax.fori_loop(0, 10, attend, 0)

    wait_for(out_w, ffn_in, ffn_out, ffn_gain_ref)

    with jax.named_scope("attended"):
        for t in range(rows // CHUNK):
            at = slice(t * CHUNK, (t + 1) * CHUNK)
            attended = jnp.concatenate(
                [
                    mixed[at, 2 * h * head : (2 * h + 1) * head] / mixed[at, (2 * h + 1) * head : 2 * (h + 1) * head]
                    for h in range(HEADS)
                ],
                axis=1,
            ).astype(bf16)
            hidden = encoded[at, :] + dot(attended, out_w[...])
            encoded[at, :] = hidden
            queries[at, :] = rms_scale(hidden, ffn_gain_ref[...])

    with jax.named_scope("expand"):
        for c in range(ffn_in.shape[1] // rows):
            cols = slice(rows * c, rows * (c + 1))
            expanded[:, cols] = silu(dot(queries[...], ffn_in[:, cols])).astype(bf16)

    with jax.named_scope("contract"):
        for t in range(rows // CHUNK):
            at = slice(t * CHUNK, (t + 1) * CHUNK)
            result_ref[at, :] = (encoded[at, :] + dot(expanded[at, :], ffn_out[...])).astype(bf16)

    for copy in land_copies + [edge_copy(k) for k in range(8)] + node_copies + [pass_on(q) for q in range(4)]:
        copy.wait_send()


def shards(
    grid_latents, mesh_latents, enc_send, enc_recv, neighbours,
    enc_grid_w, enc_bias, enc_mesh_w, enc_msg_w, upd_agg_w, upd_mesh_w, upd_out_w,
    norm_gain, query_w, key_w, value_w, out_w, ffn_gain, ffn_in_w, ffn_out_w,
):
    count = lax.axis_size("patch")
    rows, width = mesh_latents.shape
    hbm_spec = pl.BlockSpec(memory_space=pltpu.HBM)
    vmem_spec = pl.BlockSpec(memory_space=pltpu.VMEM)
    square = pltpu.VMEM((width, width), bf16)
    args = (
        grid_latents, mesh_latents, enc_send, enc_recv, neighbours.T,
        enc_grid_w, enc_bias[None, :], enc_mesh_w, enc_msg_w, upd_agg_w, upd_mesh_w, upd_out_w,
        norm_gain[None, :], query_w, key_w, value_w, out_w, ffn_gain[None, :], ffn_in_w, ffn_out_w,
    )
    return pl.pallas_call(
        functools.partial(kernel, count),
        out_shape=pltpu.VMEM((rows, width), bf16),
        in_specs=[hbm_spec] * len(args),
        out_specs=vmem_spec,
        scratch_shapes=[
            pltpu.VMEM(grid_latents.shape, bf16),
            pltpu.VMEM((rows, width), bf16),
            pltpu.VMEM(enc_send.shape, i32),
            pltpu.VMEM(enc_recv.shape, i32),
            pltpu.VMEM(neighbours.shape[::-1], i32),
            *([pltpu.VMEM((1, width), f32)] * 3),
            *([square] * 10),
            pltpu.VMEM(ffn_in_w.shape, bf16),
            pltpu.VMEM(ffn_out_w.shape, bf16),
            pltpu.VMEM(grid_latents.shape, bf16),
            pltpu.VMEM((rows, width), bf16),
            pltpu.VMEM((10, CHUNK, width), bf16),
            pltpu.VMEM((rows, width), f32),
            pltpu.VMEM((rows, width), f32),
            pltpu.VMEM((rows, width), f32),
            pltpu.VMEM((18, CHUNK, width), bf16),
            pltpu.VMEM((20, LANES, width), bf16),
            pltpu.VMEM((10, rows, CHUNK), f32),
            pltpu.VMEM((rows, width), bf16),
            pltpu.VMEM((CHUNK, 2 * width), bf16),
            pltpu.VMEM((rows, 2 * width), f32),
            pltpu.VMEM((20, LANES, LANES), i32),
            pltpu.VMEM((20, LANES, LANES), i32),
            pltpu.VMEM((20, 1, LANES), i32),
            pltpu.VMEM((LANES, LANES), i32),
            pltpu.VMEM((5, 8, LANES), i32),
            pltpu.VMEM((5, 8, LANES), i32),
            pltpu.VMEM((rows, LANES), f32),
            pltpu.VMEM((rows // 8, 2 * LANES), f32),
            pltpu.VMEM((rows, ffn_in_w.shape[1]), bf16),
            pltpu.SemaphoreType.DMA((20,)),
            pltpu.SemaphoreType.DMA((4,)),
            pltpu.SemaphoreType.DMA((4,)),
            pltpu.SemaphoreType.DMA((8,)),
            pltpu.SemaphoreType.DMA((8,)),
            pltpu.SemaphoreType.DMA((16,)),
            pltpu.SemaphoreType.DMA((16,)),
        ],
        compiler_params=pltpu.CompilerParams(
            collective_id=0, has_side_effects=True, vmem_limit_bytes=62 * 2**20
        ),
        name="encode_attend",
    )(*args)


def solution(mesh):
    split = P(("groups", "patch"), None)
    in_specs = (split,) * 5 + (P(),) * 15
    return jax.shard_map(shards, mesh=mesh, in_specs=in_specs, out_specs=split, check_vma=False)
```

```python
import functools
import math

import jax
import jax.numpy as jnp
from jax import lax
from jax.experimental import pallas as pl
from jax.experimental.pallas import tpu as pltpu
from jax.sharding import PartitionSpec as P

HEADS = 4
REACH = 2
LANES = 128
CHUNK = 256

NORM_EPS = 1e-05
HEAD_EPS = 1e-06

OWN, SIB, OTH, FW, NF = range(5)
DELTA = {OWN: 0, SIB: 1, OTH: -1, FW: 2, NF: -2}
MIRROR = {SIB: SIB, OTH: OTH, FW: NF, NF: FW}

EDGE_SEND = [(FW, 0), (NF, 0), (FW, 1), (NF, 1), (OTH, 0), (OTH, 1), (SIB, 0), (SIB, 1), (OWN, 0), (OWN, 1)]
EDGE_USE = [(OWN, 0), (OWN, 1), (SIB, 0), (SIB, 1), (NF, 0), (FW, 0), (NF, 1), (FW, 1), (OTH, 0), (OTH, 1)]
EDGE_SLOT = {key: slot for slot, key in enumerate(EDGE_USE)}
NODE_USE = (
    [(OWN, q) for q in range(4)] + [(SIB, q) for q in range(4)]
    + [(FW, 0), (FW, 1), (OTH, 0), (OTH, 1), (FW, 2), (FW, 3), (OTH, 2), (OTH, 3)]
    + [(NF, q) for q in range(4)]
)
NODE_SLOT = {key: slot for slot, key in enumerate(NODE_USE)}

f32 = jnp.float32
bf16 = jnp.bfloat16
i32 = jnp.int32


def dot(a, b):
    return jnp.dot(a, b, preferred_element_type=f32)


def dot_last(a, b):
    return lax.dot_general(a, b, (((1,), (1,)), ((), ())), preferred_element_type=f32)


def dot_first(a, b):
    return lax.dot_general(a, b, (((0,), (0,)), ((), ())), preferred_element_type=f32)


def silu(x):
    half = 0.5 * x
    return half * jnp.tanh(half) + half


def flag(mask):
    return jnp.where(mask, 1.0, 0.0).astype(bf16)


def kernel(
    count,
    grid_hbm, mesh_hbm, send_hbm, recv_hbm, neigh_hbm,
    grid_w_hbm, bias_hbm, mesh_w_hbm, msg_w_hbm, upd_agg_hbm, upd_mesh_hbm, upd_out_hbm,
    gain_hbm, query_hbm, key_hbm, value_hbm, out_w_hbm, ffn_gain_hbm, ffn_in_hbm, ffn_out_hbm,
    result_ref,
    grid_v, mesh_v, send_ref, recv_ref, neigh_ref, bias_ref, gain_ref, ffn_gain_ref, grid_w, mesh_w, msg_w, upd_agg, upd_mesh, upd_out, query_w, key_w, value_w, out_w, ffn_in, ffn_out,
    projected, receiver, received, base, summed, encoded, edges, nodes, counts, queries, values, mixed,
    send_cols, land_cols, land_rows, stage, land_send, land_recv, hi_tiled, lo_rows, expanded,
    load_sem, ls_sem, lr_sem, es_sem, er_sem, ns_sem, nr_sem,
):
    me = lax.axis_index("patch")
    sign = 1 - 2 * (me % 2)
    device = {role: (me + sign * DELTA[role] + count) % count for role in DELTA}
    block_row = {role: 4 * (sign * DELTA[role] + REACH) for role in DELTA}
    rows = mesh_v.shape[0]

    def load(index, src, dst):
        copy = pltpu.make_async_copy(src, dst, load_sem.at[index])
        copy.start()
        return copy

    def remote(src, dst, send_sem, recv_sem, role):
        return pltpu.make_async_remote_copy(
            src_ref=src, dst_ref=dst, send_sem=send_sem, recv_sem=recv_sem,
            device_id={"patch": device[role]}, device_id_type=pl.DeviceIdType.MESH,
        )

    pairs = [
        (send_hbm, send_ref), (recv_hbm, recv_ref), (bias_hbm, bias_ref), (grid_hbm, grid_v), (grid_w_hbm, grid_w), (mesh_hbm, mesh_v), (mesh_w_hbm, mesh_w), (msg_w_hbm, msg_w),
        (upd_mesh_hbm, upd_mesh), (upd_agg_hbm, upd_agg), (upd_out_hbm, upd_out), (query_hbm, query_w),
        (gain_hbm, gain_ref), (ffn_gain_hbm, ffn_gain_ref), (neigh_hbm, neigh_ref), (key_hbm, key_w), (value_hbm, value_w), (out_w_hbm, out_w), (ffn_in_hbm, ffn_in), (ffn_out_hbm, ffn_out),
    ]
    loads = {id(dst): load(index, src, dst) for index, (src, dst) in enumerate(pairs[:5])}

    def wait_for(*refs):
        for ref in refs:
            loads[id(ref)].wait()

    barrier = pltpu.get_barrier_semaphore()
    for role in (SIB, OTH, FW, NF):
        pl.semaphore_signal(
            barrier, inc=1, device_id={"patch": device[role]}, device_id_type=pl.DeviceIdType.MESH
        )

    wait_for(send_ref, recv_ref)

    land_send[...] = jnp.zeros_like(land_send)
    stage[...] = jnp.zeros_like(stage)
    for role in DELTA:
        for j in range(4):
            land_send[role, j : j + 1, :] = recv_ref[pl.ds(block_row[role] + j, 1), :]
    for k, (role, half) in enumerate(EDGE_SEND):
        for j in range(2):
            stage[2 * k + j : 2 * k + j + 1, :] = send_ref[pl.ds(block_row[role] + 2 * half + j, 1), :]

    land_copies = [
        remote(land_send.at[role], land_recv.at[MIRROR[role]], ls_sem.at[role - 1], lr_sem.at[MIRROR[role] - 1], role)
        for role in (SIB, OTH, FW, NF)
    ]

    turned = stage[...].T
    for b in range(20):
        send_cols[b] = jnp.broadcast_to(turned[:, b : b + 1], (LANES, LANES))

    lane = lax.broadcasted_iota(i32, (4 * LANES, LANES), 1)

    def onehot(cols, k, width):
        col = jnp.concatenate([cols[4 * k + j] for j in range(4)], axis=0)
        return jnp.concatenate([flag(col == lane + LANES * t) for t in range(width // LANES)], axis=1)

    with jax.named_scope("wait_grid"):
        wait_for(grid_v, grid_w, bias_ref)
    loads |= {id(dst): load(index + 5, src, dst) for index, (src, dst) in enumerate(pairs[5:])}

    def project(t, carry):
        at = pl.ds(pl.multiple_of(t * rows, rows), rows)
        projected[at, :] = (dot(grid_v[at, :], grid_w[...]) + bias_ref[...]).astype(bf16)
        return carry

    with jax.named_scope("project"):
        lax.fori_loop(0, grid_v.shape[0] // rows, project, 0)

    def edge_copy(k):
        role, half = EDGE_SEND[k]
        slot = EDGE_SLOT[(MIRROR[role], half)]
        return remote(edges.at[10 + k], edges.at[slot], es_sem.at[k], er_sem.at[slot - 2], role)

    def pick(k, carry):
        chosen = onehot(send_cols, k, grid_v.shape[0])
        picked = dot(chosen, projected[...]).astype(bf16)
        for c in range(2):
            edges[(10 + 2 * k + c) % 18] = picked[c * CHUNK : (c + 1) * CHUNK, :]

        @pl.when(k == 0)
        def _():
            pl.semaphore_wait(barrier, 4)
            for copy in land_copies:
                copy.start()

        for index in range(4):
            @pl.when(k == index)
            def _():
                edge_copy(2 * index).start()
                edge_copy(2 * index + 1).start()
        return carry

    with jax.named_scope("pick"):
        lax.fori_loop(0, 5, pick, 0)

    wait_for(mesh_v, mesh_w, upd_mesh)

    def prepare(t, carry):
        at = pl.ds(pl.multiple_of(t * CHUNK, CHUNK), CHUNK)
        latents = mesh_v[at, :]
        receiver[at, :] = dot(latents, mesh_w[...]).astype(bf16)
        base[at, :] = dot(latents, upd_mesh[...])
        summed[at, :] = jnp.zeros((CHUNK, summed.shape[1]), f32)
        return carry

    with jax.named_scope("prepare"):
        lax.fori_loop(0, rows // CHUNK, prepare, 0)

    for role in (SIB, OTH, FW, NF):
        remote(land_send.at[role], land_recv.at[role], ls_sem.at[role - 1], lr_sem.at[role - 1], role).wait_recv()
    for i, (role, half) in enumerate(EDGE_USE):
        source = land_send if role == OWN else land_recv
        for j in range(2):
            row = source[role, 2 * half + j : 2 * half + j + 1, :]
            land_rows[2 * i + j] = row
            stage[2 * i + j : 2 * i + j + 1, :] = row
    landed = stage[...].T
    for b in range(20):
        land_cols[b] = jnp.broadcast_to(landed[:, b : b + 1], (LANES, LANES))
    wait_for(msg_w)

    def receive(i, carry):
        picked = dot(onehot(land_cols, i, rows), receiver[...]).astype(bf16)
        for c in range(2):
            received[2 * i + c] = picked[c * CHUNK : (c + 1) * CHUNK, :]
        return carry

    def use_edges(i):
        messages = []
        for c in range(2):
            active = silu(edges[2 * i + c].astype(f32) + received[2 * i + c].astype(f32)).astype(bf16)
            messages.append(dot(active, msg_w[...]).astype(bf16))
        landing = jnp.concatenate([land_rows[4 * i + j] for j in range(4)], axis=1)
        scatter = flag(lax.broadcasted_iota(i32, (rows, 2 * CHUNK), 0) == landing)
        summed[...] += dot(scatter, jnp.concatenate(messages, axis=0))

    def own_edges(i, carry):
        use_edges(i)
        return carry

    with jax.named_scope("receive"):
        lax.fori_loop(0, 5, receive, 0)
    with jax.named_scope("own_edges"):
        lax.fori_loop(0, 1, own_edges, 0)

    wait_for(neigh_ref)
    neigh = neigh_ref[...]
    owner = lax.div(neigh, i32(rows))
    row = lax.rem(neigh, i32(rows))
    step = lax.rem((owner - me) * sign + 2 * count, i32(count))
    quarter = lax.div(row, i32(LANES))
    far = jnp.zeros_like(quarter)
    for role, offset in ((FW, 2), (NF, count - 2), (OTH, count - 1)):
        for q in range(4):
            far = jnp.where((step == offset) & (quarter == q), NODE_SLOT[(role, q)], far)
    high = jnp.where(step <= 1, quarter + 4 * step, far)
    low = lax.rem(row, i32(LANES))
    links = neigh.shape[0]
    spread = flag(
        lax.rem(lax.broadcasted_iota(i32, (links, LANES), 1), i32(links))
        == lax.broadcasted_iota(i32, (links, LANES), 0)
    )
    hi_tiled[...] = dot_first(high.astype(f32).astype(bf16), spread)
    lo_tiled = dot_first(low.astype(f32).astype(bf16), spread)
    place = lax.rem(lax.broadcasted_iota(i32, (rows, LANES), 0), i32(8))
    node_piece = lax.div(lax.broadcasted_iota(i32, (rows, LANES), 1), i32(links))
    alone = jnp.concatenate(
        [
            jnp.where(node_piece == place, lo_tiled, 0.0).astype(bf16),
            jnp.where(node_piece + LANES // links == place, lo_tiled, 0.0).astype(bf16),
        ],
        axis=1,
    )
    group = flag(
        lax.div(lax.broadcasted_iota(i32, (rows // 8, rows), 1), i32(8))
        == lax.broadcasted_iota(i32, (rows // 8, rows), 0)
    )
    lo_rows[...] = dot(group, alone)
    sub8 = lax.broadcasted_iota(i32, (8, LANES), 0)
    piece = lax.div(lax.broadcasted_iota(i32, (8, LANES), 1), i32(links))
    first = piece == sub8
    second = piece + LANES // links == sub8
    low_id = lax.broadcasted_iota(i32, (LANES, 2 * LANES), 0).astype(f32)

    def count_group(g, carry):
        at = pl.ds(pl.multiple_of(8 * g, 8), 8)
        h8 = hi_tiled[at, :]
        key = jnp.concatenate([jnp.where(first, h8, -1.0), jnp.where(second, h8, -1.0)], axis=1)
        by_high = jnp.concatenate([jnp.where(key == float(v), 1.0, 0.0) for v in range(20)], axis=0).astype(bf16)
        by_low = flag(low_id == lo_rows[pl.ds(g, 1), :])
        found = dot_last(by_high, by_low)
        for v in range(20):
            counts[v // 4, at, (v % 4) * LANES : (v % 4 + 1) * LANES] = found[8 * v : 8 * v + 8, :]
        return carry

    with jax.named_scope("count"):
        lax.fori_loop(0, rows // 8, count_group, 0, unroll=8)

    def far_edges(i, carry):
        with jax.named_scope("wait_edges"):
            for c in range(2):
                remote(
                    edges.at[2 * i + c], edges.at[2 * i + c], es_sem.at[0], er_sem.at[2 * i + c - 2], SIB
                ).wait_recv()
        with jax.named_scope("use_edges"):
            use_edges(i)
        return carry

    with jax.named_scope("far_edges"):
        lax.fori_loop(1, 5, far_edges, 0)

    wait_for(upd_agg, upd_out, query_w, gain_ref)

    def node_copy(index, role, q):
        slot = NODE_SLOT[(MIRROR[role], q)]
        return remote(nodes.at[NODE_SLOT[(OWN, q)]], nodes.at[slot], ns_sem.at[index], nr_sem.at[slot - 4], role)

    head = rows // HEADS
    query_scale = math.log2(math.e) / math.sqrt(head)

    def unit(x, scale):
        parts = []
        for h in range(HEADS):
            part = x[:, h * head : (h + 1) * head]
            square = jnp.mean(part * part, axis=-1, keepdims=True)
            parts.append((part * (lax.rsqrt(square + HEAD_EPS) * scale)).astype(bf16))
        return jnp.concatenate(parts, axis=1)

    def rms_scale(x, gain):
        square = jnp.mean(x * x, axis=-1, keepdims=True)
        return (x * lax.rsqrt(square + NORM_EPS) * gain).astype(bf16)

    node_copies = []
    for c in range(2):
        with jax.named_scope("update"):
            at = slice(c * CHUNK, (c + 1) * CHUNK)
            update = silu(dot(summed[at, :].astype(bf16), upd_agg[...]) + base[at, :]).astype(bf16)
            latent = mesh_v[at, :].astype(f32) + dot(update, upd_out[...])
            encoded[at, :] = latent
            normed = rms_scale(latent, gain_ref[...])
            for q in (2 * c, 2 * c + 1):
                nodes[q] = normed[(q - 2 * c) * LANES : (q - 2 * c + 1) * LANES, :]
                node_copies += [node_copy(3 * q + index, role, q) for index, role in enumerate((NF, SIB, FW))]
                for copy in node_copies[-3:-1]:
                    copy.start()
    with jax.named_scope("queries"):
        for c in range(2):
            at = slice(c * CHUNK, (c + 1) * CHUNK)
            own = jnp.concatenate([nodes[2 * c], nodes[2 * c + 1]], axis=0)
            queries[at, :] = unit(dot(own, query_w[...]), query_scale)
    mixed[...] = jnp.zeros_like(mixed)
    values[...] = jnp.ones_like(values)
    wait_for(key_w, value_w)

    def pass_on(q):
        source, slot = NODE_SLOT[(FW, q)], NODE_SLOT[(OTH, q)]
        return remote(nodes.at[source], nodes.at[slot], ns_sem.at[12 + q], nr_sem.at[slot - 4], SIB)

    def arrived(slot):
        remote(nodes.at[slot], nodes.at[slot], ns_sem.at[0], nr_sem.at[slot - 4], SIB).wait_recv()

    def wait_nodes(i):
        for step_index in range(1, 5):
            @pl.when(i == step_index)
            def _():
                for role, q in NODE_USE[4 * step_index : 4 * step_index + 4]:
                    arrived(NODE_SLOT[(role, q)])
                    if role == FW:
                        pass_on(q).start()

    def attend(i, carry):
        @pl.when(i == 1)
        def _():
            for q in range(4):
                node_copies[3 * q + 2].start()

        with jax.named_scope("wait_nodes"):
            wait_nodes(i)
        with jax.named_scope("attend_one"):
            attend_one(i)
        return carry

    def attend_one(i):
        features = jnp.concatenate([nodes[4 * i + j] for j in range(4)], axis=0)
        keys = unit(dot(features, key_w[...]), 1.0)
        value = dot(features, value_w[...]).astype(bf16)
        for h in range(HEADS):
            values[:, 2 * h * head : (2 * h + 1) * head] = value[:, h * head : (h + 1) * head]
        for t in range(rows // CHUNK):
            at = slice(t * CHUNK, (t + 1) * CHUNK)
            often = counts[i, at, :]
            for h in range(HEADS):
                cols = slice(h * head, (h + 1) * head)
                score = dot_last(queries[at, cols], keys[:, cols])
                weight = (jnp.exp2(score) * often).astype(bf16)
                wide = slice(2 * h * head, 2 * (h + 1) * head)
                mixed[at, wide] += dot(weight, values[:, wide])

    with jax.named_scope("attend"):
        lax.fori_loop(0, 5, attend, 0)

    wait_for(out_w, ffn_in, ffn_out, ffn_gain_ref)

    with jax.named_scope("attended"):
        for t in range(rows // CHUNK):
            at = slice(t * CHUNK, (t + 1) * CHUNK)
            attended = jnp.concatenate(
                [
                    mixed[at, 2 * h * head : (2 * h + 1) * head] / mixed[at, (2 * h + 1) * head : 2 * (h + 1) * head]
                    for h in range(HEADS)
                ],
                axis=1,
            ).astype(bf16)
            hidden = encoded[at, :] + dot(attended, out_w[...])
            encoded[at, :] = hidden
            queries[at, :] = rms_scale(hidden, ffn_gain_ref[...])

    with jax.named_scope("expand"):
        for c in range(ffn_in.shape[1] // rows):
            cols = slice(rows * c, rows * (c + 1))
            expanded[:, cols] = silu(dot(queries[...], ffn_in[:, cols])).astype(bf16)

    with jax.named_scope("contract"):
        for t in range(rows // CHUNK):
            at = slice(t * CHUNK, (t + 1) * CHUNK)
            result_ref[at, :] = (encoded[at, :] + dot(expanded[at, :], ffn_out[...])).astype(bf16)

    for copy in land_copies + [edge_copy(k) for k in range(8)] + node_copies + [pass_on(q) for q in range(4)]:
        copy.wait_send()


def shards(
    grid_latents, mesh_latents, enc_send, enc_recv, neighbours,
    enc_grid_w, enc_bias, enc_mesh_w, enc_msg_w, upd_agg_w, upd_mesh_w, upd_out_w,
    norm_gain, query_w, key_w, value_w, out_w, ffn_gain, ffn_in_w, ffn_out_w,
):
    count = lax.axis_size("patch")
    rows, width = mesh_latents.shape
    hbm_spec = pl.BlockSpec(memory_space=pltpu.HBM)
    vmem_spec = pl.BlockSpec(memory_space=pltpu.VMEM)
    square = pltpu.VMEM((width, width), bf16)
    args = (
        grid_latents, mesh_latents, enc_send, enc_recv, neighbours.T,
        enc_grid_w, enc_bias[None, :], enc_mesh_w, enc_msg_w, upd_agg_w, upd_mesh_w, upd_out_w,
        norm_gain[None, :], query_w, key_w, value_w, out_w, ffn_gain[None, :], ffn_in_w, ffn_out_w,
    )
    return pl.pallas_call(
        functools.partial(kernel, count),
        out_shape=pltpu.VMEM((rows, width), bf16),
        in_specs=[hbm_spec] * len(args),
        out_specs=vmem_spec,
        scratch_shapes=[
            pltpu.VMEM(grid_latents.shape, bf16),
            pltpu.VMEM((rows, width), bf16),
            pltpu.VMEM(enc_send.shape, i32),
            pltpu.VMEM(enc_recv.shape, i32),
            pltpu.VMEM(neighbours.shape[::-1], i32),
            *([pltpu.VMEM((1, width), f32)] * 3),
            *([square] * 10),
            pltpu.VMEM(ffn_in_w.shape, bf16),
            pltpu.VMEM(ffn_out_w.shape, bf16),
            pltpu.VMEM(grid_latents.shape, bf16),
            pltpu.VMEM((rows, width), bf16),
            pltpu.VMEM((10, CHUNK, width), bf16),
            pltpu.VMEM((rows, width), f32),
            pltpu.VMEM((rows, width), f32),
            pltpu.VMEM((rows, width), f32),
            pltpu.VMEM((18, CHUNK, width), bf16),
            pltpu.VMEM((20, LANES, width), bf16),
            pltpu.VMEM((5, rows, 4 * LANES), f32),
            pltpu.VMEM((rows, width), bf16),
            pltpu.VMEM((4 * LANES, 2 * width), bf16),
            pltpu.VMEM((rows, 2 * width), f32),
            pltpu.VMEM((20, LANES, LANES), i32),
            pltpu.VMEM((20, LANES, LANES), i32),
            pltpu.VMEM((20, 1, LANES), i32),
            pltpu.VMEM((LANES, LANES), i32),
            pltpu.VMEM((5, 8, LANES), i32),
            pltpu.VMEM((5, 8, LANES), i32),
            pltpu.VMEM((rows, LANES), f32),
            pltpu.VMEM((rows // 8, 2 * LANES), f32),
            pltpu.VMEM((rows, ffn_in_w.shape[1]), bf16),
            pltpu.SemaphoreType.DMA((20,)),
            pltpu.SemaphoreType.DMA((4,)),
            pltpu.SemaphoreType.DMA((4,)),
            pltpu.SemaphoreType.DMA((8,)),
            pltpu.SemaphoreType.DMA((8,)),
            pltpu.SemaphoreType.DMA((16,)),
            pltpu.SemaphoreType.DMA((16,)),
        ],
        compiler_params=pltpu.CompilerParams(
            collective_id=0, has_side_effects=True, vmem_limit_bytes=62 * 2**20
        ),
        name="encode_attend",
    )(*args)


def solution(mesh):
    split = P(("groups", "patch"), None)
    in_specs = (split,) * 5 + (P(),) * 15
    return jax.shard_map(shards, mesh=mesh, in_specs=in_specs, out_specs=split, check_vma=False)
```

```python
import functools
import math

import jax
import jax.numpy as jnp
from jax import lax
from jax.experimental import pallas as pl
from jax.experimental.pallas import tpu as pltpu
from jax.sharding import PartitionSpec as P

HEADS = 4
REACH = 2
LANES = 128
CHUNK = 256

NORM_EPS = 1e-05
HEAD_EPS = 1e-06

OWN, SIB, OTH, FW, NF = range(5)
DELTA = {OWN: 0, SIB: 1, OTH: -1, FW: 2, NF: -2}
MIRROR = {SIB: SIB, OTH: OTH, FW: NF, NF: FW}

EDGE_SEND = [(FW, 0), (NF, 0), (FW, 1), (NF, 1), (OTH, 0), (OTH, 1), (SIB, 0), (SIB, 1), (OWN, 0), (OWN, 1)]
EDGE_USE = [(OWN, 0), (OWN, 1), (SIB, 0), (SIB, 1), (NF, 0), (FW, 0), (NF, 1), (FW, 1), (OTH, 0), (OTH, 1)]
EDGE_SLOT = {key: slot for slot, key in enumerate(EDGE_USE)}
NODE_USE = (
    [(OWN, q) for q in range(4)] + [(SIB, q) for q in range(4)]
    + [(FW, 0), (FW, 1), (OTH, 0), (OTH, 1), (FW, 2), (NF, 0)]
    + [(OTH, 2), (NF, 1), (FW, 3), (NF, 2), (OTH, 3), (NF, 3)]
)
NODE_SLOT = {key: slot for slot, key in enumerate(NODE_USE)}

f32 = jnp.float32
bf16 = jnp.bfloat16
i32 = jnp.int32


def dot(a, b):
    return jnp.dot(a, b, preferred_element_type=f32)


def dot_last(a, b):
    return lax.dot_general(a, b, (((1,), (1,)), ((), ())), preferred_element_type=f32)


def dot_first(a, b):
    return lax.dot_general(a, b, (((0,), (0,)), ((), ())), preferred_element_type=f32)


def silu(x):
    half = 0.5 * x
    return half * jnp.tanh(half) + half


def flag(mask):
    return jnp.where(mask, 1.0, 0.0).astype(bf16)


def kernel(
    count,
    grid_hbm, mesh_hbm, send_hbm, recv_hbm, neigh_hbm,
    grid_w_hbm, bias_hbm, mesh_w_hbm, msg_w_hbm, upd_agg_hbm, upd_mesh_hbm, upd_out_hbm,
    gain_hbm, query_hbm, key_hbm, value_hbm, out_w_hbm, ffn_gain_hbm, ffn_in_hbm, ffn_out_hbm,
    result_ref,
    grid_v, mesh_v, send_ref, recv_ref, neigh_ref, bias_ref, gain_ref, ffn_gain_ref, grid_w, mesh_w, msg_w, upd_agg, upd_mesh, upd_out, query_w, key_w, value_w, out_w, ffn_in, ffn_out,
    projected, receiver, received, base, summed, encoded, edges, nodes, counts, queries, values, mixed,
    send_cols, land_cols, land_rows, stage, land_send, land_recv, hi_tiled, lo_rows, expanded,
    load_sem, ls_sem, lr_sem, es_sem, er_sem, ns_sem, nr_sem, relay_send, relay_recv,
):
    me = lax.axis_index("patch")
    sign = 1 - 2 * (me % 2)
    device = {role: (me + sign * DELTA[role] + count) % count for role in DELTA}
    block_row = {role: 4 * (sign * DELTA[role] + REACH) for role in DELTA}
    rows = mesh_v.shape[0]

    def load(index, src, dst):
        copy = pltpu.make_async_copy(src, dst, load_sem.at[index])
        copy.start()
        return copy

    def remote(src, dst, send_sem, recv_sem, role):
        return pltpu.make_async_remote_copy(
            src_ref=src, dst_ref=dst, send_sem=send_sem, recv_sem=recv_sem,
            device_id={"patch": device[role]}, device_id_type=pl.DeviceIdType.MESH,
        )

    pairs = [
        (send_hbm, send_ref), (recv_hbm, recv_ref), (bias_hbm, bias_ref), (grid_hbm, grid_v), (grid_w_hbm, grid_w), (mesh_hbm, mesh_v), (mesh_w_hbm, mesh_w), (msg_w_hbm, msg_w),
        (upd_mesh_hbm, upd_mesh), (upd_agg_hbm, upd_agg), (upd_out_hbm, upd_out), (query_hbm, query_w),
        (gain_hbm, gain_ref), (ffn_gain_hbm, ffn_gain_ref), (neigh_hbm, neigh_ref), (key_hbm, key_w), (value_hbm, value_w), (out_w_hbm, out_w), (ffn_in_hbm, ffn_in), (ffn_out_hbm, ffn_out),
    ]
    loads = {id(dst): load(index, src, dst) for index, (src, dst) in enumerate(pairs[:5])}

    def wait_for(*refs):
        for ref in refs:
            loads[id(ref)].wait()

    barrier = pltpu.get_barrier_semaphore()
    for role in (SIB, FW, NF):
        pl.semaphore_signal(
            barrier, inc=1, device_id={"patch": device[role]}, device_id_type=pl.DeviceIdType.MESH
        )

    wait_for(send_ref, recv_ref)

    land_send[...] = jnp.zeros_like(land_send)
    stage[...] = jnp.zeros_like(stage)
    for role in DELTA:
        for j in range(4):
            land_send[role, j : j + 1, :] = recv_ref[pl.ds(block_row[role] + j, 1), :]
    for k, (role, half) in enumerate(EDGE_SEND):
        for j in range(2):
            stage[2 * k + j : 2 * k + j + 1, :] = send_ref[pl.ds(block_row[role] + 2 * half + j, 1), :]

    land_copies = [
        remote(land_send.at[role], land_recv.at[MIRROR[role]], ls_sem.at[role - 1], lr_sem.at[MIRROR[role] - 1], role)
        for role in (SIB, FW, NF)
    ]
    land_copies.append(remote(land_send.at[OTH], land_recv.at[OWN], ls_sem.at[OTH - 1], relay_recv.at[2], SIB))
    land_relay = remote(land_recv.at[OWN], land_recv.at[OTH], relay_send.at[2], lr_sem.at[OTH - 1], FW)

    turned = stage[...].T
    for b in range(20):
        send_cols[b] = jnp.broadcast_to(turned[:, b : b + 1], (LANES, LANES))

    lane = lax.broadcasted_iota(i32, (4 * LANES, LANES), 1)

    def onehot(cols, k, width):
        col = jnp.concatenate([cols[4 * k + j] for j in range(4)], axis=0)
        return jnp.concatenate([flag(col == lane + LANES * t) for t in range(width // LANES)], axis=1)

    with jax.named_scope("wait_grid"):
        wait_for(grid_v, grid_w, bias_ref)
    loads |= {id(dst): load(index + 5, src, dst) for index, (src, dst) in enumerate(pairs[5:])}

    def project(t, carry):
        at = pl.ds(pl.multiple_of(t * rows, rows), rows)
        projected[at, :] = project_rows(grid_v[at, :])
        return carry

    def edge_copy(k):
        role, half = EDGE_SEND[k]
        if role == OTH:
            return remote(edges.at[10 + k], edges.at[18 + half], es_sem.at[k], relay_recv.at[half], SIB)
        slot = EDGE_SLOT[(MIRROR[role], half)]
        return remote(edges.at[10 + k], edges.at[slot], es_sem.at[k], er_sem.at[slot - 2], role)

    def edge_relay(half):
        slot = EDGE_SLOT[(OTH, half)]
        return remote(edges.at[18 + half], edges.at[slot], relay_send.at[half], er_sem.at[slot - 2], FW)

    def relay_arrived(index, buffer):
        remote(buffer, buffer, es_sem.at[0], relay_recv.at[index], SIB).wait_recv()

    def pick_first():
        picked = dot(onehot(send_cols, 0, grid_v.shape[0]), grid_v[...]).astype(bf16)
        for c in range(2):
            edges[10 + c] = picked[c * CHUNK : (c + 1) * CHUNK, :]

    with jax.named_scope("pick_first"):
        pick_first()
        pl.semaphore_wait(barrier, 3)
        for copy in land_copies:
            copy.start()
        for k in range(2):
            edge_copy(k).start()

    def project_rows(values):
        return (dot(values, grid_w[...]) + bias_ref[...]).astype(bf16)

    with jax.named_scope("project"):
        lax.fori_loop(0, grid_v.shape[0] // rows, project, 0)

    with jax.named_scope("relay_rows"):
        relay_arrived(2, land_recv.at[OWN])
        land_relay.start()

    def pick(k, carry):
        chosen = onehot(send_cols, k, grid_v.shape[0])
        picked = dot(chosen, projected[...]).astype(bf16)
        for c in range(2):
            edges[(10 + 2 * k + c) % 18] = picked[c * CHUNK : (c + 1) * CHUNK, :]

        for index in range(1, 4):
            @pl.when(k == index)
            def _():
                edge_copy(2 * index).start()
                edge_copy(2 * index + 1).start()
        return carry

    with jax.named_scope("pick"):
        lax.fori_loop(1, 5, pick, 0)

    with jax.named_scope("relay_edges"):
        for half in range(2):
            relay_arrived(half, edges.at[18 + half])
            edge_relay(half).start()

    wait_for(mesh_v, mesh_w, upd_mesh)

    def prepare(t, carry):
        at = pl.ds(pl.multiple_of(t * CHUNK, CHUNK), CHUNK)
        latents = mesh_v[at, :]
        receiver[at, :] = dot(latents, mesh_w[...]).astype(bf16)
        base[at, :] = dot(latents, upd_mesh[...])
        summed[at, :] = jnp.zeros((CHUNK, summed.shape[1]), f32)
        return carry

    with jax.named_scope("prepare"):
        lax.fori_loop(0, rows // CHUNK, prepare, 0)

    def place_receivers(pairs):
        for i in pairs:
            role, half = EDGE_USE[i]
            if role != OWN and half == 0:
                remote(
                    land_send.at[role], land_recv.at[role], ls_sem.at[role - 1], lr_sem.at[role - 1], role
                ).wait_recv()
            source = land_send if role == OWN else land_recv
            for j in range(2):
                row = source[role, 2 * half + j : 2 * half + j + 1, :]
                land_rows[2 * i + j] = row
                stage[2 * i + j : 2 * i + j + 1, :] = row
        landed = stage[...].T
        for i in pairs:
            for b in (2 * i, 2 * i + 1):
                land_cols[b] = jnp.broadcast_to(landed[:, b : b + 1], (LANES, LANES))

    place_receivers(range(8))
    wait_for(msg_w)

    def receive(i, carry):
        picked = dot(onehot(land_cols, i, rows), receiver[...]).astype(bf16)
        for c in range(2):
            received[2 * i + c] = picked[c * CHUNK : (c + 1) * CHUNK, :]
        return carry

    def use_edges(i):
        messages = []
        for c in range(2):
            active = silu(edges[2 * i + c].astype(f32) + received[2 * i + c].astype(f32)).astype(bf16)
            messages.append(dot(active, msg_w[...]).astype(bf16))
        landing = jnp.concatenate([land_rows[4 * i + j] for j in range(4)], axis=1)
        scatter = flag(lax.broadcasted_iota(i32, (rows, 2 * CHUNK), 0) == landing)
        summed[...] += dot(scatter, jnp.concatenate(messages, axis=0))

    def own_edges(i, carry):
        use_edges(i)
        return carry

    with jax.named_scope("receive"):
        lax.fori_loop(0, 4, receive, 0)
    with jax.named_scope("own_edges"):
        lax.fori_loop(0, 1, own_edges, 0)

    wait_for(neigh_ref)
    neigh = neigh_ref[...]
    owner = lax.div(neigh, i32(rows))
    row = lax.rem(neigh, i32(rows))
    step = lax.rem((owner - me) * sign + 2 * count, i32(count))
    quarter = lax.div(row, i32(LANES))
    far = jnp.zeros_like(quarter)
    for role, offset in ((FW, 2), (NF, count - 2), (OTH, count - 1)):
        for q in range(4):
            far = jnp.where((step == offset) & (quarter == q), NODE_SLOT[(role, q)], far)
    high = jnp.where(step <= 1, quarter + 4 * step, far)
    low = lax.rem(row, i32(LANES))
    links = neigh.shape[0]
    spread = flag(
        lax.rem(lax.broadcasted_iota(i32, (links, LANES), 1), i32(links))
        == lax.broadcasted_iota(i32, (links, LANES), 0)
    )
    hi_tiled[...] = dot_first(high.astype(f32).astype(bf16), spread)
    lo_tiled = dot_first(low.astype(f32).astype(bf16), spread)
    place = lax.rem(lax.broadcasted_iota(i32, (rows, LANES), 0), i32(8))
    node_piece = lax.div(lax.broadcasted_iota(i32, (rows, LANES), 1), i32(links))
    alone = jnp.concatenate(
        [
            jnp.where(node_piece == place, lo_tiled, 0.0).astype(bf16),
            jnp.where(node_piece + LANES // links == place, lo_tiled, 0.0).astype(bf16),
        ],
        axis=1,
    )
    group = flag(
        lax.div(lax.broadcasted_iota(i32, (rows // 8, rows), 1), i32(8))
        == lax.broadcasted_iota(i32, (rows // 8, rows), 0)
    )
    lo_rows[...] = dot(group, alone)
    sub8 = lax.broadcasted_iota(i32, (8, LANES), 0)
    piece = lax.div(lax.broadcasted_iota(i32, (8, LANES), 1), i32(links))
    first = piece == sub8
    second = piece + LANES // links == sub8
    low_id = lax.broadcasted_iota(i32, (LANES, 2 * LANES), 0).astype(f32)

    def count_group(g, carry):
        at = pl.ds(pl.multiple_of(8 * g, 8), 8)
        h8 = hi_tiled[at, :]
        key = jnp.concatenate([jnp.where(first, h8, -1.0), jnp.where(second, h8, -1.0)], axis=1)
        by_high = jnp.concatenate([jnp.where(key == float(v), 1.0, 0.0) for v in range(20)], axis=0).astype(bf16)
        by_low = flag(low_id == lo_rows[pl.ds(g, 1), :])
        found = dot_last(by_high, by_low)
        for v in range(20):
            counts[v // 2, at, (v % 2) * LANES : (v % 2 + 1) * LANES] = found[8 * v : 8 * v + 8, :]
        return carry

    with jax.named_scope("count"):
        lax.fori_loop(0, rows // 8, count_group, 0, unroll=8)

    def far_edges(i, carry):
        with jax.named_scope("wait_edges"):
            for c in range(2):
                remote(
                    edges.at[2 * i + c], edges.at[2 * i + c], es_sem.at[0], er_sem.at[2 * i + c - 2], SIB
                ).wait_recv()
        @pl.when(i == 2)
        def _():
            for c in range(2):
                edges[4 + c] = project_rows(edges[4 + c])

        with jax.named_scope("use_edges"):
            use_edges(i)
        return carry

    with jax.named_scope("receive_last"):
        place_receivers((8, 9))
        receive(4, 0)
    with jax.named_scope("far_edges"):
        lax.fori_loop(1, 5, far_edges, 0)

    wait_for(upd_agg, upd_out, query_w, gain_ref)

    def node_copy(index, role, q):
        slot = NODE_SLOT[(MIRROR[role], q)]
        return remote(nodes.at[NODE_SLOT[(OWN, q)]], nodes.at[slot], ns_sem.at[index], nr_sem.at[slot - 4], role)

    head = rows // HEADS
    query_scale = math.log2(math.e) / math.sqrt(head)

    def unit(x, scale):
        parts = []
        for h in range(HEADS):
            part = x[:, h * head : (h + 1) * head]
            square = jnp.mean(part * part, axis=-1, keepdims=True)
            parts.append((part * (lax.rsqrt(square + HEAD_EPS) * scale)).astype(bf16))
        return jnp.concatenate(parts, axis=1)

    def rms_scale(x, gain):
        square = jnp.mean(x * x, axis=-1, keepdims=True)
        return (x * lax.rsqrt(square + NORM_EPS) * gain).astype(bf16)

    node_copies = []
    for c in range(2):
        with jax.named_scope("update"):
            at = slice(c * CHUNK, (c + 1) * CHUNK)
            update = silu(dot(summed[at, :].astype(bf16), upd_agg[...]) + base[at, :]).astype(bf16)
            latent = mesh_v[at, :].astype(f32) + dot(update, upd_out[...])
            encoded[at, :] = latent
            normed = rms_scale(latent, gain_ref[...])
            for q in (2 * c, 2 * c + 1):
                nodes[q] = normed[(q - 2 * c) * LANES : (q - 2 * c + 1) * LANES, :]
                node_copies += [node_copy(3 * q + index, role, q) for index, role in enumerate((NF, SIB, FW))]
                for copy in node_copies[-3:-1]:
                    copy.start()
    with jax.named_scope("queries"):
        for c in range(2):
            at = slice(c * CHUNK, (c + 1) * CHUNK)
            own = jnp.concatenate([nodes[2 * c], nodes[2 * c + 1]], axis=0)
            queries[at, :] = unit(dot(own, query_w[...]), query_scale)
    mixed[...] = jnp.zeros_like(mixed)
    values[...] = jnp.ones_like(values)
    wait_for(key_w, value_w)

    def pass_on(q):
        source, slot = NODE_SLOT[(FW, q)], NODE_SLOT[(OTH, q)]
        return remote(nodes.at[source], nodes.at[slot], ns_sem.at[12 + q], nr_sem.at[slot - 4], SIB)

    def arrived(slot):
        remote(nodes.at[slot], nodes.at[slot], ns_sem.at[0], nr_sem.at[slot - 4], SIB).wait_recv()

    def wait_nodes(blocks):
        for role, q in blocks:
            arrived(NODE_SLOT[(role, q)])
            if role == FW:
                pass_on(q).start()

    def attend(block, pairs):
        size = 2 * pairs * LANES
        features = jnp.concatenate([nodes[block + j] for j in range(2 * pairs)], axis=0)
        keys = unit(dot(features, key_w[...]), 1.0)
        value = dot(features, value_w[...]).astype(bf16)
        for h in range(HEADS):
            values[:size, 2 * h * head : (2 * h + 1) * head] = value[:, h * head : (h + 1) * head]
        for t in range(rows // CHUNK):
            at = slice(t * CHUNK, (t + 1) * CHUNK)
            often = jnp.concatenate([counts[block // 2 + j, at, :] for j in range(pairs)], axis=1)
            for h in range(HEADS):
                cols = slice(h * head, (h + 1) * head)
                score = dot_last(queries[at, cols], keys[:, cols])
                weight = (jnp.exp2(score) * often).astype(bf16)
                wide = slice(2 * h * head, 2 * (h + 1) * head)
                mixed[at, wide] += dot(weight, values[:size, wide])

    def attend_chip(i, carry):
        @pl.when(i == 1)
        def _():
            with jax.named_scope("wait_sib"):
                wait_nodes(NODE_USE[4:8])

        with jax.named_scope("attend_four"):
            attend(4 * i, 2)
        return carry

    def attend_far(i, carry):
        with jax.named_scope("wait_nodes"):
            for index in range(6):
                @pl.when(i == index)
                def _():
                    wait_nodes(NODE_USE[8 + 2 * index : 10 + 2 * index])

        with jax.named_scope("attend_two"):
            attend(8 + 2 * i, 1)
        return carry

    with jax.named_scope("attend_chip"):
        lax.fori_loop(0, 2, attend_chip, 0)
    for q in range(4):
        node_copies[3 * q + 2].start()
    with jax.named_scope("attend"):
        lax.fori_loop(0, 6, attend_far, 0)

    wait_for(out_w, ffn_in, ffn_out, ffn_gain_ref)

    with jax.named_scope("attended"):
        for t in range(rows // CHUNK):
            at = slice(t * CHUNK, (t + 1) * CHUNK)
            attended = jnp.concatenate(
                [
                    mixed[at, 2 * h * head : (2 * h + 1) * head] / mixed[at, (2 * h + 1) * head : 2 * (h + 1) * head]
                    for h in range(HEADS)
                ],
                axis=1,
            ).astype(bf16)
            hidden = encoded[at, :] + dot(attended, out_w[...])
            encoded[at, :] = hidden
            queries[at, :] = rms_scale(hidden, ffn_gain_ref[...])

    with jax.named_scope("expand"):
        for c in range(ffn_in.shape[1] // rows):
            cols = slice(rows * c, rows * (c + 1))
            expanded[:, cols] = silu(dot(queries[...], ffn_in[:, cols])).astype(bf16)

    with jax.named_scope("contract"):
        for t in range(rows // CHUNK):
            at = slice(t * CHUNK, (t + 1) * CHUNK)
            result_ref[at, :] = (encoded[at, :] + dot(expanded[at, :], ffn_out[...])).astype(bf16)

    for copy in land_copies + [edge_copy(k) for k in range(8)] + node_copies + [pass_on(q) for q in range(4)] + [land_relay, edge_relay(0), edge_relay(1)]:
        copy.wait_send()


def shards(
    grid_latents, mesh_latents, enc_send, enc_recv, neighbours,
    enc_grid_w, enc_bias, enc_mesh_w, enc_msg_w, upd_agg_w, upd_mesh_w, upd_out_w,
    norm_gain, query_w, key_w, value_w, out_w, ffn_gain, ffn_in_w, ffn_out_w,
):
    count = lax.axis_size("patch")
    rows, width = mesh_latents.shape
    hbm_spec = pl.BlockSpec(memory_space=pltpu.HBM)
    vmem_spec = pl.BlockSpec(memory_space=pltpu.VMEM)
    square = pltpu.VMEM((width, width), bf16)
    args = (
        grid_latents, mesh_latents, enc_send, enc_recv, neighbours.T,
        enc_grid_w, enc_bias[None, :], enc_mesh_w, enc_msg_w, upd_agg_w, upd_mesh_w, upd_out_w,
        norm_gain[None, :], query_w, key_w, value_w, out_w, ffn_gain[None, :], ffn_in_w, ffn_out_w,
    )
    return pl.pallas_call(
        functools.partial(kernel, count),
        out_shape=pltpu.VMEM((rows, width), bf16),
        in_specs=[hbm_spec] * len(args),
        out_specs=vmem_spec,
        scratch_shapes=[
            pltpu.VMEM(grid_latents.shape, bf16),
            pltpu.VMEM((rows, width), bf16),
            pltpu.VMEM(enc_send.shape, i32),
            pltpu.VMEM(enc_recv.shape, i32),
            pltpu.VMEM(neighbours.shape[::-1], i32),
            *([pltpu.VMEM((1, width), f32)] * 3),
            *([square] * 10),
            pltpu.VMEM(ffn_in_w.shape, bf16),
            pltpu.VMEM(ffn_out_w.shape, bf16),
            pltpu.VMEM(grid_latents.shape, bf16),
            pltpu.VMEM((rows, width), bf16),
            pltpu.VMEM((10, CHUNK, width), bf16),
            pltpu.VMEM((rows, width), f32),
            pltpu.VMEM((rows, width), f32),
            pltpu.VMEM((rows, width), f32),
            pltpu.VMEM((20, CHUNK, width), bf16),
            pltpu.VMEM((20, LANES, width), bf16),
            pltpu.VMEM((10, rows, 2 * LANES), f32),
            pltpu.VMEM((rows, width), bf16),
            pltpu.VMEM((4 * LANES, 2 * width), bf16),
            pltpu.VMEM((rows, 2 * width), f32),
            pltpu.VMEM((20, LANES, LANES), i32),
            pltpu.VMEM((20, LANES, LANES), i32),
            pltpu.VMEM((20, 1, LANES), i32),
            pltpu.VMEM((LANES, LANES), i32),
            pltpu.VMEM((5, 8, LANES), i32),
            pltpu.VMEM((5, 8, LANES), i32),
            pltpu.VMEM((rows, LANES), f32),
            pltpu.VMEM((rows // 8, 2 * LANES), f32),
            pltpu.VMEM((rows, ffn_in_w.shape[1]), bf16),
            pltpu.SemaphoreType.DMA((20,)),
            pltpu.SemaphoreType.DMA((4,)),
            pltpu.SemaphoreType.DMA((4,)),
            pltpu.SemaphoreType.DMA((8,)),
            pltpu.SemaphoreType.DMA((8,)),
            pltpu.SemaphoreType.DMA((16,)),
            pltpu.SemaphoreType.DMA((16,)),
            pltpu.SemaphoreType.DMA((3,)),
            pltpu.SemaphoreType.DMA((3,)),
        ],
        compiler_params=pltpu.CompilerParams(
            collective_id=0, has_side_effects=True, vmem_limit_bytes=62 * 2**20
        ),
        name="encode_attend",
    )(*args)


def solution(mesh):
    split = P(("groups", "patch"), None)
    in_specs = (split,) * 5 + (P(),) * 15
    return jax.shard_map(shards, mesh=mesh, in_specs=in_specs, out_specs=split, check_vma=False)
```

```python
import functools
import math

import jax
import jax.numpy as jnp
from jax import lax
from jax.experimental import pallas as pl
from jax.experimental.pallas import tpu as pltpu
from jax.sharding import PartitionSpec as P

HEADS = 4
REACH = 2
LANES = 128
CHUNK = 256

NORM_EPS = 1e-05
HEAD_EPS = 1e-06

OWN, SIB, OTH, FW, NF = range(5)
DELTA = {OWN: 0, SIB: 1, OTH: -1, FW: 2, NF: -2}
MIRROR = {SIB: SIB, OTH: OTH, FW: NF, NF: FW}

EDGE_SEND = [(FW, 0), (NF, 0), (FW, 1), (NF, 1), (OTH, 0), (OTH, 1), (SIB, 0), (SIB, 1), (OWN, 0), (OWN, 1)]
EDGE_USE = [(OWN, 0), (OWN, 1), (SIB, 0), (SIB, 1), (NF, 0), (FW, 0), (NF, 1), (FW, 1), (OTH, 0), (OTH, 1)]
EDGE_SLOT = {key: slot for slot, key in enumerate(EDGE_USE)}
NODE_USE = (
    [(OWN, q) for q in range(4)] + [(SIB, q) for q in range(4)]
    + [(FW, 0), (FW, 1), (OTH, 0), (OTH, 1), (FW, 2), (NF, 0)]
    + [(OTH, 2), (NF, 1), (FW, 3), (NF, 2), (OTH, 3), (NF, 3)]
)
NODE_SLOT = {key: slot for slot, key in enumerate(NODE_USE)}

f32 = jnp.float32
bf16 = jnp.bfloat16
i32 = jnp.int32


def dot(a, b):
    return jnp.dot(a, b, preferred_element_type=f32)


def dot_last(a, b):
    return lax.dot_general(a, b, (((1,), (1,)), ((), ())), preferred_element_type=f32)


def dot_first(a, b):
    return lax.dot_general(a, b, (((0,), (0,)), ((), ())), preferred_element_type=f32)


def silu(x):
    half = 0.5 * x
    return half * jnp.tanh(half) + half


def flag(mask):
    return jnp.where(mask, 1.0, 0.0).astype(bf16)


def kernel(
    count,
    grid_hbm, mesh_hbm, send_hbm, recv_hbm, neigh_hbm,
    grid_w_hbm, bias_hbm, mesh_w_hbm, msg_w_hbm, upd_agg_hbm, upd_mesh_hbm, upd_out_hbm,
    gain_hbm, query_hbm, key_hbm, value_hbm, out_w_hbm, ffn_gain_hbm, ffn_in_hbm, ffn_out_hbm,
    result_ref,
    grid_v, mesh_v, send_ref, recv_ref, neigh_ref, bias_ref, gain_ref, ffn_gain_ref, grid_w, mesh_w, msg_w, upd_agg, upd_mesh, upd_out, query_w, key_w, value_w, out_w, ffn_in, ffn_out,
    projected, receiver, received, base, summed, encoded, edges, nodes, counts, queries, values, mixed,
    send_cols, land_cols, land_rows, stage, land_send, land_recv, hi_tiled, lo_rows, expanded,
    load_sem, ls_sem, lr_sem, es_sem, er_sem, ns_sem, nr_sem, relay_send, relay_recv,
):
    me = lax.axis_index("patch")
    sign = 1 - 2 * (me % 2)
    device = {role: (me + sign * DELTA[role] + count) % count for role in DELTA}
    block_row = {role: 4 * (sign * DELTA[role] + REACH) for role in DELTA}
    rows = mesh_v.shape[0]

    def load(index, src, dst):
        copy = pltpu.make_async_copy(src, dst, load_sem.at[index])
        copy.start()
        return copy

    def remote(src, dst, send_sem, recv_sem, role):
        return pltpu.make_async_remote_copy(
            src_ref=src, dst_ref=dst, send_sem=send_sem, recv_sem=recv_sem,
            device_id={"patch": device[role]}, device_id_type=pl.DeviceIdType.MESH,
        )

    pairs = [
        (send_hbm, send_ref), (recv_hbm, recv_ref), (bias_hbm, bias_ref), (grid_hbm, grid_v), (grid_w_hbm, grid_w), (mesh_hbm, mesh_v), (mesh_w_hbm, mesh_w), (msg_w_hbm, msg_w),
        (upd_mesh_hbm, upd_mesh), (upd_agg_hbm, upd_agg), (upd_out_hbm, upd_out), (query_hbm, query_w),
        (gain_hbm, gain_ref), (ffn_gain_hbm, ffn_gain_ref), (neigh_hbm, neigh_ref), (key_hbm, key_w), (value_hbm, value_w), (out_w_hbm, out_w), (ffn_in_hbm, ffn_in), (ffn_out_hbm, ffn_out),
    ]
    loads = {id(dst): load(index, src, dst) for index, (src, dst) in enumerate(pairs[:5])}

    def wait_for(*refs):
        for ref in refs:
            loads[id(ref)].wait()

    barrier = pltpu.get_barrier_semaphore()
    for role in (SIB, FW, NF):
        pl.semaphore_signal(
            barrier, inc=1, device_id={"patch": device[role]}, device_id_type=pl.DeviceIdType.MESH
        )

    wait_for(send_ref, recv_ref)

    land_send[...] = jnp.zeros_like(land_send)
    stage[...] = jnp.zeros_like(stage)
    for role in DELTA:
        for j in range(4):
            land_send[role, j : j + 1, :] = recv_ref[pl.ds(block_row[role] + j, 1), :]
    for k, (role, half) in enumerate(EDGE_SEND):
        for j in range(2):
            stage[2 * k + j : 2 * k + j + 1, :] = send_ref[pl.ds(block_row[role] + 2 * half + j, 1), :]

    land_copies = [
        remote(land_send.at[role], land_recv.at[MIRROR[role]], ls_sem.at[role - 1], lr_sem.at[MIRROR[role] - 1], role)
        for role in (SIB, FW, NF)
    ]
    land_copies.append(remote(land_send.at[OTH], land_recv.at[OWN], ls_sem.at[OTH - 1], relay_recv.at[2], SIB))
    land_relay = remote(land_recv.at[OWN], land_recv.at[OTH], relay_send.at[2], lr_sem.at[OTH - 1], FW)

    turned = stage[...].T
    for b in range(20):
        send_cols[b] = jnp.broadcast_to(turned[:, b : b + 1], (LANES, LANES))

    lane = lax.broadcasted_iota(i32, (4 * LANES, LANES), 1)

    def onehot(cols, k, width):
        col = jnp.concatenate([cols[4 * k + j] for j in range(4)], axis=0)
        return jnp.concatenate([flag(col == lane + LANES * t) for t in range(width // LANES)], axis=1)

    with jax.named_scope("wait_grid"):
        wait_for(grid_v, grid_w, bias_ref)
    loads |= {id(dst): load(index + 5, src, dst) for index, (src, dst) in enumerate(pairs[5:])}

    def project(t, carry):
        at = pl.ds(pl.multiple_of(t * rows, rows), rows)
        projected[at, :] = project_rows(grid_v[at, :])
        return carry

    def edge_copy(k):
        role, half = EDGE_SEND[k]
        if role == OTH:
            return remote(edges.at[10 + k], edges.at[18 + half], es_sem.at[k], relay_recv.at[half], SIB)
        slot = EDGE_SLOT[(MIRROR[role], half)]
        return remote(edges.at[10 + k], edges.at[slot], es_sem.at[k], er_sem.at[slot - 2], role)

    def edge_relay(half):
        slot = EDGE_SLOT[(OTH, half)]
        return remote(edges.at[18 + half], edges.at[slot], relay_send.at[half], er_sem.at[slot - 2], FW)

    def relay_arrived(index, buffer):
        remote(buffer, buffer, es_sem.at[0], relay_recv.at[index], SIB).wait_recv()

    def pick_first():
        picked = dot(onehot(send_cols, 0, grid_v.shape[0]), grid_v[...]).astype(bf16)
        for c in range(2):
            edges[10 + c] = picked[c * CHUNK : (c + 1) * CHUNK, :]

    with jax.named_scope("pick_first"):
        pick_first()
        pl.semaphore_wait(barrier, 3)
        for copy in land_copies:
            copy.start()
        for k in range(2):
            edge_copy(k).start()

    def project_rows(values):
        return (dot(values, grid_w[...]) + bias_ref[...]).astype(bf16)

    with jax.named_scope("project"):
        lax.fori_loop(0, grid_v.shape[0] // rows, project, 0)

    def pick(k, carry):
        chosen = onehot(send_cols, k, grid_v.shape[0])
        picked = dot(chosen, projected[...]).astype(bf16)
        for c in range(2):
            edges[(10 + 2 * k + c) % 18] = picked[c * CHUNK : (c + 1) * CHUNK, :]

        for index in range(1, 4):
            @pl.when(k == index)
            def _():
                edge_copy(2 * index).start()
                edge_copy(2 * index + 1).start()
        return carry

    with jax.named_scope("pick"):
        lax.fori_loop(1, 5, pick, 0)

    wait_for(mesh_v, mesh_w, upd_mesh)

    def prepare(t, carry):
        at = pl.ds(pl.multiple_of(t * CHUNK, CHUNK), CHUNK)
        latents = mesh_v[at, :]
        receiver[at, :] = dot(latents, mesh_w[...]).astype(bf16)
        base[at, :] = dot(latents, upd_mesh[...])
        summed[at, :] = jnp.zeros((CHUNK, summed.shape[1]), f32)
        return carry

    with jax.named_scope("prepare"):
        lax.fori_loop(0, rows // CHUNK, prepare, 0)

    wait_for(neigh_ref)
    neigh = neigh_ref[...]
    owner = lax.div(neigh, i32(rows))
    row = lax.rem(neigh, i32(rows))
    step = lax.rem((owner - me) * sign + 2 * count, i32(count))
    quarter = lax.div(row, i32(LANES))
    far = jnp.zeros_like(quarter)
    for role, offset in ((FW, 2), (NF, count - 2), (OTH, count - 1)):
        for q in range(4):
            far = jnp.where((step == offset) & (quarter == q), NODE_SLOT[(role, q)], far)
    high = jnp.where(step <= 1, quarter + 4 * step, far)
    low = lax.rem(row, i32(LANES))
    links = neigh.shape[0]
    spread = flag(
        lax.rem(lax.broadcasted_iota(i32, (links, LANES), 1), i32(links))
        == lax.broadcasted_iota(i32, (links, LANES), 0)
    )
    hi_tiled[...] = dot_first(high.astype(f32).astype(bf16), spread)
    lo_tiled = dot_first(low.astype(f32).astype(bf16), spread)
    place = lax.rem(lax.broadcasted_iota(i32, (rows, LANES), 0), i32(8))
    node_piece = lax.div(lax.broadcasted_iota(i32, (rows, LANES), 1), i32(links))
    alone = jnp.concatenate(
        [
            jnp.where(node_piece == place, lo_tiled, 0.0).astype(bf16),
            jnp.where(node_piece + LANES // links == place, lo_tiled, 0.0).astype(bf16),
        ],
        axis=1,
    )
    group = flag(
        lax.div(lax.broadcasted_iota(i32, (rows // 8, rows), 1), i32(8))
        == lax.broadcasted_iota(i32, (rows // 8, rows), 0)
    )
    lo_rows[...] = dot(group, alone)
    sub8 = lax.broadcasted_iota(i32, (8, LANES), 0)
    piece = lax.div(lax.broadcasted_iota(i32, (8, LANES), 1), i32(links))
    first = piece == sub8
    second = piece + LANES // links == sub8
    low_id = lax.broadcasted_iota(i32, (LANES, 2 * LANES), 0).astype(f32)

    def count_group(g, carry):
        at = pl.ds(pl.multiple_of(8 * g, 8), 8)
        h8 = hi_tiled[at, :]
        key = jnp.concatenate([jnp.where(first, h8, -1.0), jnp.where(second, h8, -1.0)], axis=1)
        by_high = jnp.concatenate([jnp.where(key == float(v), 1.0, 0.0) for v in range(20)], axis=0).astype(bf16)
        by_low = flag(low_id == lo_rows[pl.ds(g, 1), :])
        found = dot_last(by_high, by_low)
        for v in range(20):
            counts[v // 2, at, (v % 2) * LANES : (v % 2 + 1) * LANES] = found[8 * v : 8 * v + 8, :]
        return carry

    with jax.named_scope("count"):
        lax.fori_loop(0, rows // 8, count_group, 0, unroll=8)

    with jax.named_scope("relay_rows"):
        relay_arrived(2, land_recv.at[OWN])
        land_relay.start()

    with jax.named_scope("relay_edges"):
        for half in range(2):
            relay_arrived(half, edges.at[18 + half])
            edge_relay(half).start()

    def place_receivers(pairs):
        for i in pairs:
            role, half = EDGE_USE[i]
            if role != OWN and half == 0:
                remote(
                    land_send.at[role], land_recv.at[role], ls_sem.at[role - 1], lr_sem.at[role - 1], role
                ).wait_recv()
            source = land_send if role == OWN else land_recv
            for j in range(2):
                row = source[role, 2 * half + j : 2 * half + j + 1, :]
                land_rows[2 * i + j] = row
                stage[2 * i + j : 2 * i + j + 1, :] = row
        landed = stage[...].T
        for i in pairs:
            for b in (2 * i, 2 * i + 1):
                land_cols[b] = jnp.broadcast_to(landed[:, b : b + 1], (LANES, LANES))

    place_receivers(range(8))
    wait_for(msg_w)

    def receive(i, carry):
        picked = dot(onehot(land_cols, i, rows), receiver[...]).astype(bf16)
        for c in range(2):
            received[2 * i + c] = picked[c * CHUNK : (c + 1) * CHUNK, :]
        return carry

    def use_edges(i):
        messages = []
        for c in range(2):
            active = silu(edges[2 * i + c].astype(f32) + received[2 * i + c].astype(f32)).astype(bf16)
            messages.append(dot(active, msg_w[...]).astype(bf16))
        landing = jnp.concatenate([land_rows[4 * i + j] for j in range(4)], axis=1)
        scatter = flag(lax.broadcasted_iota(i32, (rows, 2 * CHUNK), 0) == landing)
        summed[...] += dot(scatter, jnp.concatenate(messages, axis=0))

    def own_edges(i, carry):
        use_edges(i)
        return carry

    with jax.named_scope("receive"):
        lax.fori_loop(0, 4, receive, 0)
    with jax.named_scope("own_edges"):
        lax.fori_loop(0, 1, own_edges, 0)

    def far_edges(i, carry):
        with jax.named_scope("wait_edges"):
            for c in range(2):
                remote(
                    edges.at[2 * i + c], edges.at[2 * i + c], es_sem.at[0], er_sem.at[2 * i + c - 2], SIB
                ).wait_recv()
        @pl.when(i == 2)
        def _():
            for c in range(2):
                edges[4 + c] = project_rows(edges[4 + c])

        with jax.named_scope("use_edges"):
            use_edges(i)
        return carry

    with jax.named_scope("receive_last"):
        place_receivers((8, 9))
        receive(4, 0)
    with jax.named_scope("far_edges"):
        lax.fori_loop(1, 5, far_edges, 0)

    wait_for(upd_agg, upd_out, query_w, gain_ref)

    def node_copy(index, role, q):
        slot = NODE_SLOT[(MIRROR[role], q)]
        return remote(nodes.at[NODE_SLOT[(OWN, q)]], nodes.at[slot], ns_sem.at[index], nr_sem.at[slot - 4], role)

    head = rows // HEADS
    query_scale = math.log2(math.e) / math.sqrt(head)

    def unit(x, scale):
        parts = []
        for h in range(HEADS):
            part = x[:, h * head : (h + 1) * head]
            square = jnp.mean(part * part, axis=-1, keepdims=True)
            parts.append((part * (lax.rsqrt(square + HEAD_EPS) * scale)).astype(bf16))
        return jnp.concatenate(parts, axis=1)

    def rms_scale(x, gain):
        square = jnp.mean(x * x, axis=-1, keepdims=True)
        return (x * lax.rsqrt(square + NORM_EPS) * gain).astype(bf16)

    node_copies = []
    for c in range(2):
        with jax.named_scope("update"):
            at = slice(c * CHUNK, (c + 1) * CHUNK)
            update = silu(dot(summed[at, :].astype(bf16), upd_agg[...]) + base[at, :]).astype(bf16)
            latent = mesh_v[at, :].astype(f32) + dot(update, upd_out[...])
            encoded[at, :] = latent
            normed = rms_scale(latent, gain_ref[...])
            for q in (2 * c, 2 * c + 1):
                nodes[q] = normed[(q - 2 * c) * LANES : (q - 2 * c + 1) * LANES, :]
                node_copies += [node_copy(3 * q + index, role, q) for index, role in enumerate((NF, SIB, FW))]
                for copy in node_copies[-3:-1]:
                    copy.start()
    with jax.named_scope("queries"):
        for c in range(2):
            at = slice(c * CHUNK, (c + 1) * CHUNK)
            own = jnp.concatenate([nodes[2 * c], nodes[2 * c + 1]], axis=0)
            queries[at, :] = unit(dot(own, query_w[...]), query_scale)
    mixed[...] = jnp.zeros_like(mixed)
    values[...] = jnp.ones_like(values)
    wait_for(key_w, value_w)

    def pass_on(q):
        source, slot = NODE_SLOT[(FW, q)], NODE_SLOT[(OTH, q)]
        return remote(nodes.at[source], nodes.at[slot], ns_sem.at[12 + q], nr_sem.at[slot - 4], SIB)

    def arrived(slot):
        remote(nodes.at[slot], nodes.at[slot], ns_sem.at[0], nr_sem.at[slot - 4], SIB).wait_recv()

    def wait_nodes(blocks):
        for role, q in blocks:
            arrived(NODE_SLOT[(role, q)])
            if role == FW:
                pass_on(q).start()

    def attend(block, pairs):
        size = 2 * pairs * LANES
        features = jnp.concatenate([nodes[block + j] for j in range(2 * pairs)], axis=0)
        keys = unit(dot(features, key_w[...]), 1.0)
        value = dot(features, value_w[...]).astype(bf16)
        for h in range(HEADS):
            values[:size, 2 * h * head : (2 * h + 1) * head] = value[:, h * head : (h + 1) * head]
        for t in range(rows // CHUNK):
            at = slice(t * CHUNK, (t + 1) * CHUNK)
            often = jnp.concatenate([counts[block // 2 + j, at, :] for j in range(pairs)], axis=1)
            for h in range(HEADS):
                cols = slice(h * head, (h + 1) * head)
                score = dot_last(queries[at, cols], keys[:, cols])
                weight = (jnp.exp2(score) * often).astype(bf16)
                wide = slice(2 * h * head, 2 * (h + 1) * head)
                mixed[at, wide] += dot(weight, values[:size, wide])

    def attend_chip(i, carry):
        @pl.when(i == 1)
        def _():
            with jax.named_scope("wait_sib"):
                wait_nodes(NODE_USE[4:8])

        with jax.named_scope("attend_four"):
            attend(4 * i, 2)
        return carry

    def attend_far(i, carry):
        with jax.named_scope("wait_nodes"):
            for index in range(6):
                @pl.when(i == index)
                def _():
                    wait_nodes(NODE_USE[8 + 2 * index : 10 + 2 * index])

        with jax.named_scope("attend_two"):
            attend(8 + 2 * i, 1)
        return carry

    with jax.named_scope("attend_chip"):
        lax.fori_loop(0, 2, attend_chip, 0)
    for q in range(4):
        node_copies[3 * q + 2].start()
    with jax.named_scope("attend"):
        lax.fori_loop(0, 6, attend_far, 0)

    wait_for(out_w, ffn_in, ffn_out, ffn_gain_ref)

    with jax.named_scope("attended"):
        for t in range(rows // CHUNK):
            at = slice(t * CHUNK, (t + 1) * CHUNK)
            attended = jnp.concatenate(
                [
                    mixed[at, 2 * h * head : (2 * h + 1) * head] / mixed[at, (2 * h + 1) * head : 2 * (h + 1) * head]
                    for h in range(HEADS)
                ],
                axis=1,
            ).astype(bf16)
            hidden = encoded[at, :] + dot(attended, out_w[...])
            encoded[at, :] = hidden
            queries[at, :] = rms_scale(hidden, ffn_gain_ref[...])

    with jax.named_scope("expand"):
        for c in range(ffn_in.shape[1] // rows):
            cols = slice(rows * c, rows * (c + 1))
            expanded[:, cols] = silu(dot(queries[...], ffn_in[:, cols])).astype(bf16)

    with jax.named_scope("contract"):
        for t in range(rows // CHUNK):
            at = slice(t * CHUNK, (t + 1) * CHUNK)
            result_ref[at, :] = (encoded[at, :] + dot(expanded[at, :], ffn_out[...])).astype(bf16)

    for copy in land_copies + [edge_copy(k) for k in range(8)] + node_copies + [pass_on(q) for q in range(4)] + [land_relay, edge_relay(0), edge_relay(1)]:
        copy.wait_send()


def shards(
    grid_latents, mesh_latents, enc_send, enc_recv, neighbours,
    enc_grid_w, enc_bias, enc_mesh_w, enc_msg_w, upd_agg_w, upd_mesh_w, upd_out_w,
    norm_gain, query_w, key_w, value_w, out_w, ffn_gain, ffn_in_w, ffn_out_w,
):
    count = lax.axis_size("patch")
    rows, width = mesh_latents.shape
    hbm_spec = pl.BlockSpec(memory_space=pltpu.HBM)
    vmem_spec = pl.BlockSpec(memory_space=pltpu.VMEM)
    square = pltpu.VMEM((width, width), bf16)
    args = (
        grid_latents, mesh_latents, enc_send, enc_recv, neighbours.T,
        enc_grid_w, enc_bias[None, :], enc_mesh_w, enc_msg_w, upd_agg_w, upd_mesh_w, upd_out_w,
        norm_gain[None, :], query_w, key_w, value_w, out_w, ffn_gain[None, :], ffn_in_w, ffn_out_w,
    )
    return pl.pallas_call(
        functools.partial(kernel, count),
        out_shape=pltpu.VMEM((rows, width), bf16),
        in_specs=[hbm_spec] * len(args),
        out_specs=vmem_spec,
        scratch_shapes=[
            pltpu.VMEM(grid_latents.shape, bf16),
            pltpu.VMEM((rows, width), bf16),
            pltpu.VMEM(enc_send.shape, i32),
            pltpu.VMEM(enc_recv.shape, i32),
            pltpu.VMEM(neighbours.shape[::-1], i32),
            *([pltpu.VMEM((1, width), f32)] * 3),
            *([square] * 10),
            pltpu.VMEM(ffn_in_w.shape, bf16),
            pltpu.VMEM(ffn_out_w.shape, bf16),
            pltpu.VMEM(grid_latents.shape, bf16),
            pltpu.VMEM((rows, width), bf16),
            pltpu.VMEM((10, CHUNK, width), bf16),
            pltpu.VMEM((rows, width), f32),
            pltpu.VMEM((rows, width), f32),
            pltpu.VMEM((rows, width), f32),
            pltpu.VMEM((20, CHUNK, width), bf16),
            pltpu.VMEM((20, LANES, width), bf16),
            pltpu.VMEM((10, rows, 2 * LANES), f32),
            pltpu.VMEM((rows, width), bf16),
            pltpu.VMEM((4 * LANES, 2 * width), bf16),
            pltpu.VMEM((rows, 2 * width), f32),
            pltpu.VMEM((20, LANES, LANES), i32),
            pltpu.VMEM((20, LANES, LANES), i32),
            pltpu.VMEM((20, 1, LANES), i32),
            pltpu.VMEM((LANES, LANES), i32),
            pltpu.VMEM((5, 8, LANES), i32),
            pltpu.VMEM((5, 8, LANES), i32),
            pltpu.VMEM((rows, LANES), f32),
            pltpu.VMEM((rows // 8, 2 * LANES), f32),
            pltpu.VMEM((rows, ffn_in_w.shape[1]), bf16),
            pltpu.SemaphoreType.DMA((20,)),
            pltpu.SemaphoreType.DMA((4,)),
            pltpu.SemaphoreType.DMA((4,)),
            pltpu.SemaphoreType.DMA((8,)),
            pltpu.SemaphoreType.DMA((8,)),
            pltpu.SemaphoreType.DMA((16,)),
            pltpu.SemaphoreType.DMA((16,)),
            pltpu.SemaphoreType.DMA((3,)),
            pltpu.SemaphoreType.DMA((3,)),
        ],
        compiler_params=pltpu.CompilerParams(
            collective_id=0, has_side_effects=True, vmem_limit_bytes=62 * 2**20
        ),
        name="encode_attend",
    )(*args)


def solution(mesh):
    split = P(("groups", "patch"), None)
    in_specs = (split,) * 5 + (P(),) * 15
    return jax.shard_map(shards, mesh=mesh, in_specs=in_specs, out_specs=split, check_vma=False)
```

```python
import functools
import math

import jax
import jax.numpy as jnp
from jax import lax
from jax.experimental import pallas as pl
from jax.experimental.pallas import tpu as pltpu
from jax.sharding import PartitionSpec as P

HEADS = 4
REACH = 2
LANES = 128
CHUNK = 256

NORM_EPS = 1e-05
HEAD_EPS = 1e-06

OWN, SIB, OTH, FW, NF = range(5)
DELTA = {OWN: 0, SIB: 1, OTH: -1, FW: 2, NF: -2}
MIRROR = {SIB: SIB, OTH: OTH, FW: NF, NF: FW}

EDGE_SEND = [(FW, 0), (NF, 0), (FW, 1), (NF, 1), (OTH, 0), (OTH, 1), (SIB, 0), (SIB, 1), (OWN, 0), (OWN, 1)]
EDGE_USE = [(OWN, 0), (OWN, 1), (SIB, 0), (SIB, 1), (NF, 0), (FW, 0), (NF, 1), (FW, 1), (OTH, 0), (OTH, 1)]
EDGE_SLOT = {key: slot for slot, key in enumerate(EDGE_USE)}
NODE_USE = (
    [(OWN, q) for q in range(4)] + [(SIB, q) for q in range(4)]
    + [(FW, 0), (FW, 1), (OTH, 0), (OTH, 1), (FW, 2), (NF, 0)]
    + [(OTH, 2), (NF, 1), (FW, 3), (NF, 2), (OTH, 3), (NF, 3)]
)
NODE_SLOT = {key: slot for slot, key in enumerate(NODE_USE)}

f32 = jnp.float32
bf16 = jnp.bfloat16
i32 = jnp.int32


def dot(a, b):
    return jnp.dot(a, b, preferred_element_type=f32)


def dot_last(a, b):
    return lax.dot_general(a, b, (((1,), (1,)), ((), ())), preferred_element_type=f32)


def dot_first(a, b):
    return lax.dot_general(a, b, (((0,), (0,)), ((), ())), preferred_element_type=f32)


def silu(x):
    half = 0.5 * x
    return half * jnp.tanh(half) + half


def flag(mask):
    return jnp.where(mask, 1.0, 0.0).astype(bf16)


def kernel(
    count,
    grid_hbm, mesh_hbm, send_hbm, recv_hbm, neigh_hbm,
    grid_w_hbm, bias_hbm, mesh_w_hbm, msg_w_hbm, upd_agg_hbm, upd_mesh_hbm, upd_out_hbm,
    gain_hbm, query_hbm, key_hbm, value_hbm, out_w_hbm, ffn_gain_hbm, ffn_in_hbm, ffn_out_hbm,
    result_ref,
    grid_v, mesh_v, send_ref, recv_ref, neigh_ref, bias_ref, gain_ref, ffn_gain_ref, grid_w, mesh_w, msg_w, upd_agg, upd_mesh, upd_out, query_w, key_w, value_w, out_w, ffn_in, ffn_out,
    projected, receiver, received, base, summed, encoded, edges, nodes, counts, queries, values, mixed,
    send_cols, land_cols, land_rows, stage, land_send, land_recv, hi_tiled, lo_rows, expanded,
    load_sem, ls_sem, lr_sem, es_sem, er_sem, ns_sem, nr_sem, relay_send, relay_recv,
):
    me = lax.axis_index("patch")
    sign = 1 - 2 * (me % 2)
    device = {role: (me + sign * DELTA[role] + count) % count for role in DELTA}
    block_row = {role: 4 * (sign * DELTA[role] + REACH) for role in DELTA}
    rows = mesh_v.shape[0]

    def load(index, src, dst):
        copy = pltpu.make_async_copy(src, dst, load_sem.at[index])
        copy.start()
        return copy

    def remote(src, dst, send_sem, recv_sem, role):
        return pltpu.make_async_remote_copy(
            src_ref=src, dst_ref=dst, send_sem=send_sem, recv_sem=recv_sem,
            device_id={"patch": device[role]}, device_id_type=pl.DeviceIdType.MESH,
        )

    pairs = [
        (send_hbm, send_ref), (recv_hbm, recv_ref), (bias_hbm, bias_ref), (grid_hbm, grid_v), (grid_w_hbm, grid_w), (mesh_hbm, mesh_v), (mesh_w_hbm, mesh_w), (msg_w_hbm, msg_w),
        (upd_mesh_hbm, upd_mesh), (upd_agg_hbm, upd_agg), (upd_out_hbm, upd_out), (query_hbm, query_w),
        (gain_hbm, gain_ref), (ffn_gain_hbm, ffn_gain_ref), (neigh_hbm, neigh_ref), (key_hbm, key_w), (value_hbm, value_w), (out_w_hbm, out_w), (ffn_in_hbm, ffn_in), (ffn_out_hbm, ffn_out),
    ]
    loads = {id(dst): load(index, src, dst) for index, (src, dst) in enumerate(pairs[:5])}

    def wait_for(*refs):
        for ref in refs:
            loads[id(ref)].wait()

    barrier = pltpu.get_barrier_semaphore()
    for role in (SIB, FW, NF):
        pl.semaphore_signal(
            barrier, inc=1, device_id={"patch": device[role]}, device_id_type=pl.DeviceIdType.MESH
        )

    wait_for(send_ref, recv_ref)

    land_send[...] = jnp.zeros_like(land_send)
    stage[...] = jnp.zeros_like(stage)
    for role in DELTA:
        for j in range(4):
            land_send[role, j : j + 1, :] = recv_ref[pl.ds(block_row[role] + j, 1), :]
    for k, (role, half) in enumerate(EDGE_SEND):
        for j in range(2):
            stage[2 * k + j : 2 * k + j + 1, :] = send_ref[pl.ds(block_row[role] + 2 * half + j, 1), :]

    land_copies = [
        remote(land_send.at[role], land_recv.at[MIRROR[role]], ls_sem.at[role - 1], lr_sem.at[MIRROR[role] - 1], role)
        for role in (SIB, FW, NF)
    ]
    land_copies.append(remote(land_send.at[OTH], land_recv.at[OWN], ls_sem.at[OTH - 1], relay_recv.at[2], SIB))
    land_relay = remote(land_recv.at[OWN], land_recv.at[OTH], relay_send.at[2], lr_sem.at[OTH - 1], FW)

    turned = stage[...].T
    for b in range(20):
        send_cols[b] = jnp.broadcast_to(turned[:, b : b + 1], (LANES, LANES))

    lane = lax.broadcasted_iota(i32, (4 * LANES, LANES), 1)

    def onehot(cols, k, width):
        col = jnp.concatenate([cols[4 * k + j] for j in range(4)], axis=0)
        return jnp.concatenate([flag(col == lane + LANES * t) for t in range(width // LANES)], axis=1)

    with jax.named_scope("wait_grid"):
        wait_for(grid_v, grid_w, bias_ref)
    loads |= {id(dst): load(index + 5, src, dst) for index, (src, dst) in enumerate(pairs[5:])}

    def project(t, carry):
        at = pl.ds(pl.multiple_of(t * rows, rows), rows)
        projected[at, :] = project_rows(grid_v[at, :])
        return carry

    def edge_copy(k):
        role, half = EDGE_SEND[k]
        if role == OTH:
            return remote(edges.at[10 + k], edges.at[18 + half], es_sem.at[k], relay_recv.at[half], SIB)
        slot = EDGE_SLOT[(MIRROR[role], half)]
        return remote(edges.at[10 + k], edges.at[slot], es_sem.at[k], er_sem.at[slot - 2], role)

    def edge_relay(half):
        slot = EDGE_SLOT[(OTH, half)]
        return remote(edges.at[18 + half], edges.at[slot], relay_send.at[half], er_sem.at[slot - 2], FW)

    def relay_arrived(index, buffer):
        remote(buffer, buffer, es_sem.at[0], relay_recv.at[index], SIB).wait_recv()

    def pick_first():
        picked = dot(onehot(send_cols, 0, grid_v.shape[0]), grid_v[...]).astype(bf16)
        for c in range(2):
            edges[10 + c] = picked[c * CHUNK : (c + 1) * CHUNK, :]

    with jax.named_scope("pick_first"):
        pick_first()
        pl.semaphore_wait(barrier, 3)
        for copy in land_copies:
            copy.start()
        for k in range(2):
            edge_copy(k).start()

    def project_rows(values):
        return (dot(values, grid_w[...]) + bias_ref[...]).astype(bf16)

    with jax.named_scope("project"):
        lax.fori_loop(0, grid_v.shape[0] // rows, project, 0)

    def pick(k, carry):
        chosen = onehot(send_cols, k, grid_v.shape[0])
        picked = dot(chosen, projected[...]).astype(bf16)
        for c in range(2):
            edges[(10 + 2 * k + c) % 18] = picked[c * CHUNK : (c + 1) * CHUNK, :]

        for index in range(1, 4):
            @pl.when(k == index)
            def _():
                edge_copy(2 * index).start()
                edge_copy(2 * index + 1).start()
        return carry

    with jax.named_scope("pick"):
        lax.fori_loop(1, 5, pick, 0)

    wait_for(mesh_v, mesh_w, upd_mesh)

    def prepare(t, carry):
        at = pl.ds(pl.multiple_of(t * CHUNK, CHUNK), CHUNK)
        latents = mesh_v[at, :]
        receiver[at, :] = dot(latents, mesh_w[...]).astype(bf16)
        base[at, :] = dot(latents, upd_mesh[...])
        summed[at, :] = jnp.zeros((CHUNK, summed.shape[1]), f32)
        return carry

    with jax.named_scope("prepare"):
        lax.fori_loop(0, rows // CHUNK, prepare, 0)

    wait_for(neigh_ref)
    neigh = neigh_ref[...]
    owner = lax.div(neigh, i32(rows))
    row = lax.rem(neigh, i32(rows))
    step = lax.rem((owner - me) * sign + 2 * count, i32(count))
    quarter = lax.div(row, i32(LANES))
    far = jnp.zeros_like(quarter)
    for role, offset in ((FW, 2), (NF, count - 2), (OTH, count - 1)):
        for q in range(4):
            far = jnp.where((step == offset) & (quarter == q), NODE_SLOT[(role, q)], far)
    high = jnp.where(step <= 1, quarter + 4 * step, far)
    low = lax.rem(row, i32(LANES))
    links = neigh.shape[0]
    spread = flag(
        lax.rem(lax.broadcasted_iota(i32, (links, LANES), 1), i32(links))
        == lax.broadcasted_iota(i32, (links, LANES), 0)
    )
    hi_tiled[...] = dot_first(high.astype(f32).astype(bf16), spread)
    lo_tiled = dot_first(low.astype(f32).astype(bf16), spread)
    place = lax.rem(lax.broadcasted_iota(i32, (rows, LANES), 0), i32(8))
    node_piece = lax.div(lax.broadcasted_iota(i32, (rows, LANES), 1), i32(links))
    alone = jnp.concatenate(
        [
            jnp.where(node_piece == place, lo_tiled, 0.0).astype(bf16),
            jnp.where(node_piece + LANES // links == place, lo_tiled, 0.0).astype(bf16),
        ],
        axis=1,
    )
    group = flag(
        lax.div(lax.broadcasted_iota(i32, (rows // 8, rows), 1), i32(8))
        == lax.broadcasted_iota(i32, (rows // 8, rows), 0)
    )
    lo_rows[...] = dot(group, alone)
    sub8 = lax.broadcasted_iota(i32, (8, LANES), 0)
    piece = lax.div(lax.broadcasted_iota(i32, (8, LANES), 1), i32(links))
    first = piece == sub8
    second = piece + LANES // links == sub8
    low_id = lax.broadcasted_iota(i32, (LANES, 2 * LANES), 0).astype(f32)

    def count_group(g, carry):
        at = pl.ds(pl.multiple_of(8 * g, 8), 8)
        h8 = hi_tiled[at, :]
        key = jnp.concatenate([jnp.where(first, h8, -1.0), jnp.where(second, h8, -1.0)], axis=1)
        by_high = jnp.concatenate([jnp.where(key == float(v), 1.0, 0.0) for v in range(20)], axis=0).astype(bf16)
        by_low = flag(low_id == lo_rows[pl.ds(g, 1), :])
        found = dot_last(by_high, by_low)
        for v in range(20):
            counts[v // 2, at, (v % 2) * LANES : (v % 2 + 1) * LANES] = found[8 * v : 8 * v + 8, :]
        return carry

    with jax.named_scope("count"):
        lax.fori_loop(0, rows // 8, count_group, 0, unroll=8)

    with jax.named_scope("relay_rows"):
        relay_arrived(2, land_recv.at[OWN])
        land_relay.start()

    with jax.named_scope("relay_edges"):
        for half in range(2):
            relay_arrived(half, edges.at[18 + half])
            edge_relay(half).start()

    def place_receivers(pairs):
        for i in pairs:
            role, half = EDGE_USE[i]
            if role != OWN and half == 0:
                remote(
                    land_send.at[role], land_recv.at[role], ls_sem.at[role - 1], lr_sem.at[role - 1], role
                ).wait_recv()
            source = land_send if role == OWN else land_recv
            for j in range(2):
                row = source[role, 2 * half + j : 2 * half + j + 1, :]
                land_rows[2 * i + j] = row
                stage[2 * i + j : 2 * i + j + 1, :] = row
        landed = stage[...].T
        for i in pairs:
            for b in (2 * i, 2 * i + 1):
                land_cols[b] = jnp.broadcast_to(landed[:, b : b + 1], (LANES, LANES))

    place_receivers(range(8))
    wait_for(msg_w)

    def receive(i, carry):
        picked = dot(onehot(land_cols, i, rows), receiver[...]).astype(bf16)
        for c in range(2):
            received[2 * i + c] = picked[c * CHUNK : (c + 1) * CHUNK, :]
        return carry

    def use_edges(i):
        messages = []
        for c in range(2):
            active = silu(edges[2 * i + c].astype(f32) + received[2 * i + c].astype(f32)).astype(bf16)
            messages.append(dot(active, msg_w[...]).astype(bf16))
        landing = jnp.concatenate([land_rows[4 * i + j] for j in range(4)], axis=1)
        scatter = flag(lax.broadcasted_iota(i32, (rows, 2 * CHUNK), 0) == landing)
        summed[...] += dot(scatter, jnp.concatenate(messages, axis=0))

    def own_edges(i, carry):
        use_edges(i)
        return carry

    with jax.named_scope("receive"):
        lax.fori_loop(0, 4, receive, 0)
    with jax.named_scope("own_edges"):
        lax.fori_loop(0, 1, own_edges, 0)

    def far_edges(i, carry):
        with jax.named_scope("wait_edges"):
            for c in range(2):
                remote(
                    edges.at[2 * i + c], edges.at[2 * i + c], es_sem.at[0], er_sem.at[2 * i + c - 2], SIB
                ).wait_recv()
        @pl.when(i == 2)
        def _():
            for c in range(2):
                edges[4 + c] = project_rows(edges[4 + c])

        with jax.named_scope("use_edges"):
            use_edges(i)
        return carry

    with jax.named_scope("receive_last"):
        place_receivers((8, 9))
        receive(4, 0)
    with jax.named_scope("far_edges"):
        lax.fori_loop(1, 5, far_edges, 0)

    wait_for(upd_agg, upd_out, query_w, gain_ref)

    def node_copy(index, role, q):
        slot = NODE_SLOT[(MIRROR[role], q)]
        return remote(nodes.at[NODE_SLOT[(OWN, q)]], nodes.at[slot], ns_sem.at[index], nr_sem.at[slot - 4], role)

    head = rows // HEADS
    query_scale = math.log2(math.e) / math.sqrt(head)

    def unit(x, scale):
        parts = []
        for h in range(HEADS):
            part = x[:, h * head : (h + 1) * head]
            square = jnp.mean(part * part, axis=-1, keepdims=True)
            parts.append((part * (lax.rsqrt(square + HEAD_EPS) * scale)).astype(bf16))
        return jnp.concatenate(parts, axis=1)

    def rms_scale(x, gain):
        square = jnp.mean(x * x, axis=-1, keepdims=True)
        return (x * lax.rsqrt(square + NORM_EPS) * gain).astype(bf16)

    node_copies = []
    for c in range(2):
        with jax.named_scope("update"):
            at = slice(c * CHUNK, (c + 1) * CHUNK)
            update = silu(dot(summed[at, :].astype(bf16), upd_agg[...]) + base[at, :]).astype(bf16)
            latent = mesh_v[at, :].astype(f32) + dot(update, upd_out[...])
            encoded[at, :] = latent
            normed = rms_scale(latent, gain_ref[...])
            for q in (2 * c, 2 * c + 1):
                nodes[q] = normed[(q - 2 * c) * LANES : (q - 2 * c + 1) * LANES, :]
                node_copies += [node_copy(3 * q + index, role, q) for index, role in enumerate((NF, SIB, FW))]
                for copy in node_copies[-3:-1]:
                    copy.start()
    with jax.named_scope("queries"):
        for c in range(2):
            at = slice(c * CHUNK, (c + 1) * CHUNK)
            own = jnp.concatenate([nodes[2 * c], nodes[2 * c + 1]], axis=0)
            queries[at, :] = unit(dot(own, query_w[...]), query_scale)
    mixed[...] = jnp.zeros_like(mixed)
    values[...] = jnp.ones_like(values)
    wait_for(key_w, value_w)

    def pass_on(q):
        source, slot = NODE_SLOT[(FW, q)], NODE_SLOT[(OTH, q)]
        return remote(nodes.at[source], nodes.at[slot], ns_sem.at[12 + q], nr_sem.at[slot - 4], SIB)

    def arrived(slot):
        remote(nodes.at[slot], nodes.at[slot], ns_sem.at[0], nr_sem.at[slot - 4], SIB).wait_recv()

    def wait_nodes(blocks):
        for role, q in blocks:
            if role != FW:
                arrived(NODE_SLOT[(role, q)])

    passed = {0: (0, 1), 1: (2,), 2: (3,)}

    def attend(block, pairs):
        size = 2 * pairs * LANES
        features = jnp.concatenate([nodes[block + j] for j in range(2 * pairs)], axis=0)
        keys = unit(dot(features, key_w[...]), 1.0)
        value = dot(features, value_w[...]).astype(bf16)
        for h in range(HEADS):
            values[:size, 2 * h * head : (2 * h + 1) * head] = value[:, h * head : (h + 1) * head]
        for t in range(rows // CHUNK):
            at = slice(t * CHUNK, (t + 1) * CHUNK)
            often = jnp.concatenate([counts[block // 2 + j, at, :] for j in range(pairs)], axis=1)
            for h in range(HEADS):
                cols = slice(h * head, (h + 1) * head)
                score = dot_last(queries[at, cols], keys[:, cols])
                weight = (jnp.exp2(score) * often).astype(bf16)
                wide = slice(2 * h * head, 2 * (h + 1) * head)
                mixed[at, wide] += dot(weight, values[:size, wide])

    def attend_chip(i, carry):
        @pl.when(i == 1)
        def _():
            with jax.named_scope("wait_sib"):
                wait_nodes(NODE_USE[4:8])

        with jax.named_scope("attend_four"):
            attend(4 * i, 2)
        return carry

    def attend_far(i, carry):
        with jax.named_scope("wait_nodes"):
            for index in range(6):
                @pl.when(i == index)
                def _():
                    for q in passed.get(index, ()):
                        arrived(NODE_SLOT[(FW, q)])
                        pass_on(q).start()
                    wait_nodes(NODE_USE[8 + 2 * index : 10 + 2 * index])

        with jax.named_scope("attend_two"):
            attend(8 + 2 * i, 1)
        return carry

    with jax.named_scope("attend_chip"):
        lax.fori_loop(0, 2, attend_chip, 0)
    for q in range(4):
        node_copies[3 * q + 2].start()
    with jax.named_scope("attend"):
        lax.fori_loop(0, 6, attend_far, 0)

    wait_for(out_w, ffn_in, ffn_out, ffn_gain_ref)

    with jax.named_scope("attended"):
        for t in range(rows // CHUNK):
            at = slice(t * CHUNK, (t + 1) * CHUNK)
            attended = jnp.concatenate(
                [
                    mixed[at, 2 * h * head : (2 * h + 1) * head] / mixed[at, (2 * h + 1) * head : 2 * (h + 1) * head]
                    for h in range(HEADS)
                ],
                axis=1,
            ).astype(bf16)
            hidden = encoded[at, :] + dot(attended, out_w[...])
            encoded[at, :] = hidden
            queries[at, :] = rms_scale(hidden, ffn_gain_ref[...])

    with jax.named_scope("expand"):
        for c in range(ffn_in.shape[1] // rows):
            cols = slice(rows * c, rows * (c + 1))
            expanded[:, cols] = silu(dot(queries[...], ffn_in[:, cols])).astype(bf16)

    with jax.named_scope("contract"):
        for t in range(rows // CHUNK):
            at = slice(t * CHUNK, (t + 1) * CHUNK)
            result_ref[at, :] = (encoded[at, :] + dot(expanded[at, :], ffn_out[...])).astype(bf16)

    for copy in land_copies + [edge_copy(k) for k in range(8)] + node_copies + [pass_on(q) for q in range(4)] + [land_relay, edge_relay(0), edge_relay(1)]:
        copy.wait_send()


def shards(
    grid_latents, mesh_latents, enc_send, enc_recv, neighbours,
    enc_grid_w, enc_bias, enc_mesh_w, enc_msg_w, upd_agg_w, upd_mesh_w, upd_out_w,
    norm_gain, query_w, key_w, value_w, out_w, ffn_gain, ffn_in_w, ffn_out_w,
):
    count = lax.axis_size("patch")
    rows, width = mesh_latents.shape
    hbm_spec = pl.BlockSpec(memory_space=pltpu.HBM)
    vmem_spec = pl.BlockSpec(memory_space=pltpu.VMEM)
    square = pltpu.VMEM((width, width), bf16)
    args = (
        grid_latents, mesh_latents, enc_send, enc_recv, neighbours.T,
        enc_grid_w, enc_bias[None, :], enc_mesh_w, enc_msg_w, upd_agg_w, upd_mesh_w, upd_out_w,
        norm_gain[None, :], query_w, key_w, value_w, out_w, ffn_gain[None, :], ffn_in_w, ffn_out_w,
    )
    return pl.pallas_call(
        functools.partial(kernel, count),
        out_shape=pltpu.VMEM((rows, width), bf16),
        in_specs=[hbm_spec] * len(args),
        out_specs=vmem_spec,
        scratch_shapes=[
            pltpu.VMEM(grid_latents.shape, bf16),
            pltpu.VMEM((rows, width), bf16),
            pltpu.VMEM(enc_send.shape, i32),
            pltpu.VMEM(enc_recv.shape, i32),
            pltpu.VMEM(neighbours.shape[::-1], i32),
            *([pltpu.VMEM((1, width), f32)] * 3),
            *([square] * 10),
            pltpu.VMEM(ffn_in_w.shape, bf16),
            pltpu.VMEM(ffn_out_w.shape, bf16),
            pltpu.VMEM(grid_latents.shape, bf16),
            pltpu.VMEM((rows, width), bf16),
            pltpu.VMEM((10, CHUNK, width), bf16),
            pltpu.VMEM((rows, width), f32),
            pltpu.VMEM((rows, width), f32),
            pltpu.VMEM((rows, width), f32),
            pltpu.VMEM((20, CHUNK, width), bf16),
            pltpu.VMEM((20, LANES, width), bf16),
            pltpu.VMEM((10, rows, 2 * LANES), f32),
            pltpu.VMEM((rows, width), bf16),
            pltpu.VMEM((4 * LANES, 2 * width), bf16),
            pltpu.VMEM((rows, 2 * width), f32),
            pltpu.VMEM((20, LANES, LANES), i32),
            pltpu.VMEM((20, LANES, LANES), i32),
            pltpu.VMEM((20, 1, LANES), i32),
            pltpu.VMEM((LANES, LANES), i32),
            pltpu.VMEM((5, 8, LANES), i32),
            pltpu.VMEM((5, 8, LANES), i32),
            pltpu.VMEM((rows, LANES), f32),
            pltpu.VMEM((rows // 8, 2 * LANES), f32),
            pltpu.VMEM((rows, ffn_in_w.shape[1]), bf16),
            pltpu.SemaphoreType.DMA((20,)),
            pltpu.SemaphoreType.DMA((4,)),
            pltpu.SemaphoreType.DMA((4,)),
            pltpu.SemaphoreType.DMA((8,)),
            pltpu.SemaphoreType.DMA((8,)),
            pltpu.SemaphoreType.DMA((16,)),
            pltpu.SemaphoreType.DMA((16,)),
            pltpu.SemaphoreType.DMA((3,)),
            pltpu.SemaphoreType.DMA((3,)),
        ],
        compiler_params=pltpu.CompilerParams(
            collective_id=0, has_side_effects=True, vmem_limit_bytes=62 * 2**20
        ),
        name="encode_attend",
    )(*args)


def solution(mesh):
    split = P(("groups", "patch"), None)
    in_specs = (split,) * 5 + (P(),) * 15
    return jax.shard_map(shards, mesh=mesh, in_specs=in_specs, out_specs=split, check_vma=False)
```
